32 devices in a mesh: groups: 2 (over x), ep: 8 (over z, y), section: 2 (over core).
Axes of the slice: x: 2, y: 2, z: 4, core: 2. Of those that a mesh axis runs over, the one named last changes fastest.
Arguments:
- resid: bfloat16 [2048, 4096], P(('groups', 'ep')), parts along dimension 0, may hold values from -6 to 6
- norm_gain: bfloat16 [4096], replicated, may hold values from 0.3984375 to 1.59375
- gate_logits: float32 [2048, 8], P(('groups', 'ep')), parts along dimension 0, may hold values from 0.1 to 1
- routes: int32 [2048, 8], P(('groups', 'ep')), parts along dimension 0, may hold values from 0 to 31, all different within a row; in each aligned block of 128 rows (0 to 127, 128 to 255, ...) at most 40 rows name the same one
- w_gate: bfloat16 [32, 4096, 768], P('ep', None, 'section'), may hold values from -0.09375 to 0.09375
- w_up: bfloat16 [32, 4096, 768], P('ep', None, 'section'), may hold values from -0.09375 to 0.09375
- w_down: bfloat16 [32, 768, 4096], P('ep', 'section'), may hold values from -0.21875 to 0.21875
- keys_raw: bfloat16 [2048, 512], P(('groups', 'ep'), 'section'), parts along dimension 0, may hold values from -6 to 6
- values_raw: bfloat16 [2048, 512], P(('groups', 'ep'), 'section'), parts along dimension 0, may hold values from -6 to 6
- k_gain: bfloat16 [128], replicated, may hold values from 0.25 to 1.75
- lengths: int32 [16], P(('groups', 'ep')), parts along dimension 0, may hold values from 32 to 128
- page_owner: int32 [16, 8], P(('groups', 'ep')), parts along dimension 0, may hold values from 0 to 7, as said below
- page_slot: int32 [16, 8], P(('groups', 'ep')), parts along dimension 0, may hold values from 0 to 7, as said below
Outputs:
- moe_out: bfloat16 [2048, 4096], P(('groups', 'ep'), 'section'), parts along dimension 0
- kv_cache: bfloat16 [128, 16, 2, 512], P(('groups', 'ep'), None, None, 'section'), parts along dimension 0
The draws below stay inside these ranges and needn't reach their ends.
There are 2 independent parts, one for each index of `groups`. The reference program is written for one: setup_inputs(seed, part) draws one part's arguments, and reference() takes and returns one part's arrays. A program takes and returns all parts, laid end to end along the dimension named above; an argument that names none is the same for every part. Nothing has to cross between parts.
Inputs may be any that keep to these rules, and one draw needn't show every extreme that they name: `page_owner`: each prompt sends its 8 pages to 4 different owners, exactly 2 pages to each of them; every owner receives exactly 8 pages. `page_slot`: the pages that reach one owner have different slots, so every slot of every owner is filled once.
All inputs are finite; a program needn't handle non-finite values.
Results may differ from the reference program's by a relative error of at most 0.0076.
Values may be sent and summed in bfloat16 or wider, within the bound.
No kernel may reach another device: no remote copies, remote signals or barrier semaphores. Data moves between devices by JAX's collectives and lax.ppermute only.
A program may use at most 128 MiB of HBM per device.

```python
import math
import jax
import jax.numpy as jnp
import numpy as np
from jax import lax

D = 4096
HEAD = 128
KV_HEADS = 4
TOP = 8
FF = 768
EXPERTS = 32
TOK_DEV = 128
PAGE = 16
CAP = 40
PAGES = 8
SEQS = 8
TOKENS = 1024


def page_plan(key):
    base = jax.random.fold_in(key, 4242)
    streams = jax.random.split(base, 5)
    owner_order = jax.random.permutation(streams[0], SEQS)
    source_order = jax.random.permutation(streams[1], SEQS)
    shifts = jax.random.permutation(streams[2], SEQS)[:PAGES // 2]
    group_owner = owner_order[(source_order[:, None] + shifts[None, :]) % SEQS]
    column_perm = jax.vmap(lambda sub: jax.random.permutation(sub, PAGES))(jax.random.split(streams[3], SEQS))
    owner = jnp.take_along_axis(group_owner, column_perm // 2, axis=1)
    slot_perm = jax.vmap(lambda sub: jax.random.permutation(sub, PAGES))(jax.random.split(streams[4], SEQS))
    slot = slot_perm[owner, column_perm]
    return (owner.astype(jnp.int32), slot.astype(jnp.int32))


def draw_page_owner(key, part):
    return page_plan(key)[0]


def draw_page_slot(key, part):
    return page_plan(key)[1]


def plant(values, stream_key, least, largest):
    spot = [jax.random.randint(jax.random.fold_in(stream_key, axis), (), 0, length) for axis, length in enumerate(values.shape)]
    longest = values.shape.index(max(values.shape))
    beside = spot[:longest] + [(spot[longest] + 1) % values.shape[longest]] + spot[longest + 1:]
    return values.at[tuple(spot)].set(least).at[tuple(beside)].set(largest)


def level_of(key, shape, shards, low, top_value):
    def one(dim, parts):
        steps = jax.random.uniform(jax.random.fold_in(jax.random.fold_in(key, 6), dim), (parts,), jnp.float32, low / len(shards), top_value / len(shards))
        return jnp.repeat(jnp.exp(steps), shape[dim] // parts).reshape((-1,) + (1,) * (len(shape) - dim - 1))

    level = one(*shards[0])
    for cut in shards[1:]:
        level = level * one(*cut)
    return level


def deal_out(stream_key, own, number, rows, number_of, top, limit, slope):
    sequence = jax.random.permutation(stream_key, number_of)
    packed, ordinary = shares(number_of, rows * top, limit, slope, True), shares(number_of, rows * top, limit, slope, False)
    places = jnp.arange(number_of)

    def named(sizes, offset_by):
        used = int((sizes > 0).sum())
        fixed = max(1, used // 4)
        moved = fixed + (places - fixed + offset_by * (used - fixed)) % max(1, number_of - fixed)
        return jnp.zeros((number_of,), jnp.int32).at[sequence[jnp.where(places < fixed, places, moved)]].set(jnp.asarray(sizes, jnp.int32))

    sizes = jnp.where(number % 4 == 0, named(packed, number // 4), named(ordinary, number - number // 4 - 1))
    mixed = jax.random.permutation(jax.random.fold_in(own, 3), number_of)
    source_of, sink = mixed[0:number_of // 2 * 2:2], mixed[1:number_of // 2 * 2:2]
    room = jnp.minimum(sizes[source_of] - 1, limit - sizes[sink]) // 2
    room = jnp.where((source_of == sequence[0]) | (sink == sequence[0]) | (sizes[sink] == 0), 0, jnp.maximum(room, 0))
    moved = jax.random.randint(jax.random.fold_in(own, 4), (number_of // 2,), 0, 1 << 20) % (room + 1)
    sizes = sizes.at[source_of].add(-moved).at[sink].add(moved)
    labels = jnp.searchsorted(jnp.cumsum(sizes), jnp.arange(rows * top), side="right").astype(jnp.int32)
    listing = labels.reshape(top, rows).T
    listing = listing[jax.random.permutation(jax.random.fold_in(own, 1), rows)]
    offset_by = jax.random.randint(jax.random.fold_in(own, 2), (rows, 1), 0, top)
    return jnp.take_along_axis(listing, (jnp.arange(top)[None, :] + offset_by) % top, axis=1)


def shares(number_of, total, limit, skew, full):
    loads = [(1 << 20) // math.isqrt(grade ** skew) + 1 for grade in range(1, number_of + 1)]
    largest = limit if full else min(limit, max(-(-total // number_of), total * loads[0] // sum(loads)))
    least = 1 if total - largest >= number_of - 1 else 0
    holding, spare = [largest] + [least] * (number_of - 1), total - largest - least * (number_of - 1)
    while spare > 0:
        movable = [i for i in range(1, number_of) if holding[i] < largest] or [i for i in range(1, number_of) if holding[i] < limit]
        pool, budget = sum([loads[i] for i in movable]), spare
        for i in movable:
            more = min(limit - holding[i], max(1, budget * loads[i] // pool), spare)
            holding[i] = holding[i] + more
            spare = spare - more
    return np.array(holding)


def noise(stream_key, shape, spread, bound, shards=(), kind=jnp.bfloat16):
    array = spread * jax.random.normal(stream_key, shape, jnp.float32)
    if shards:
        array = array * level_of(stream_key, shape, shards, -0.22, 0.18)
    return jnp.clip(array, -bound, bound).astype(kind)


def setup_inputs(seed: int = 0, part: int = 0) -> dict:
    arg_keys = jax.random.split(jax.random.key(seed), 14)
    part_keys = jax.random.split(jax.random.fold_in(arg_keys[13], part), 14)
    resid = noise(part_keys[0], (TOKENS, D), 1.0, 6.0, ((0, 8),))
    norm_gain = jnp.clip(1.0 + 0.12 * jax.random.normal(arg_keys[1], (D,), jnp.float32), 0.3984375, 1.59375).astype(jnp.bfloat16)
    gate_logits = jnp.clip(jnp.exp(math.log(1.0) - 2.3025851 * jax.random.uniform(part_keys[2], (TOKENS, TOP), jnp.float32) ** level_of(part_keys[2], (TOKENS, TOP), ((0, 8),), -0.2, 0.2)), 0.1, 1.0)
    routes_keys = jax.random.split(jax.random.fold_in(part_keys[3], 1), TOKENS // TOK_DEV)
    routes_turns = jax.random.permutation(jax.random.fold_in(part_keys[3], 3), TOKENS // TOK_DEV)
    routes = jax.vmap(lambda own, number: deal_out(jax.random.fold_in(part_keys[3], 2), own, number, TOK_DEV, EXPERTS, TOP, CAP, 1))(routes_keys, routes_turns).reshape((TOKENS, TOP))
    w_gate = noise(arg_keys[4], (EXPERTS, D, FF), D ** -0.5, 0.09375, ((0, 8), (2, 2)))
    w_up = noise(arg_keys[5], (EXPERTS, D, FF), D ** -0.5, 0.09375, ((0, 8), (2, 2)))
    w_down = noise(arg_keys[6], (EXPERTS, FF, D), FF ** -0.5, 0.21875, ((0, 8), (1, 2)))
    keys_raw = noise(part_keys[7], (TOKENS, KV_HEADS * HEAD), 1.0, 6.0, ((0, 8), (1, 2)))
    values_raw = noise(part_keys[8], (TOKENS, KV_HEADS * HEAD), 1.0, 6.0, ((0, 8), (1, 2)))
    k_gain = jnp.clip(1.0 + 0.15 * jax.random.normal(arg_keys[9], (HEAD,), jnp.float32), 0.25, 1.75).astype(jnp.bfloat16)
    lengths = plant(jax.random.randint(part_keys[10], (SEQS,), TOK_DEV // 4, TOK_DEV + 1), jax.random.fold_in(part_keys[10], 1), TOK_DEV // 4, TOK_DEV).astype(jnp.int32)
    page_owner = draw_page_owner(jax.random.fold_in(jax.random.fold_in(arg_keys[13], part), 71), part)
    page_slot = draw_page_slot(jax.random.fold_in(jax.random.fold_in(arg_keys[13], part), 71), part)
    return {"resid": resid, "norm_gain": norm_gain, "gate_logits": gate_logits, "routes": routes, "w_gate": w_gate, "w_up": w_up, "w_down": w_down, "keys_raw": keys_raw, "values_raw": values_raw, "k_gain": k_gain, "lengths": lengths, "page_owner": page_owner, "page_slot": page_slot}


def rms_scale(values, gain_row):
    mean_square = lax.optimization_barrier(jnp.mean(values * values, axis=-1, keepdims=True))
    return values * lax.rsqrt(mean_square + 1e-06) * gain_row

def rotate_keys(key_block, position):
    half_size = key_block.shape[-1] // 2
    frequency = jnp.exp(jnp.arange(half_size, dtype=jnp.float32) * (-2.0 / key_block.shape[-1]) * math.log(1000000.0))
    angles = position.astype(jnp.float32)[:, None, None] * frequency
    cosine = jnp.cos(angles)
    sine_part = jnp.sin(angles)
    first_half = key_block[..., :half_size]
    second = key_block[..., half_size:]
    return jnp.concatenate([first_half * cosine - second * sine_part, second * cosine + first_half * sine_part], axis=-1)

def reference(resid, norm_gain, gate_logits, routes, w_gate, w_up, w_down, keys_raw, values_raw, k_gain, lengths, page_owner, page_slot):
    total_tokens = SEQS * TOK_DEV
    token_ids = jnp.arange(total_tokens, dtype=jnp.int32)
    position = token_ids % TOK_DEV
    prompt_ids = token_ids // TOK_DEV
    is_live = position < lengths[prompt_ids]
    hidden = rms_scale(resid.astype(jnp.float32), norm_gain.astype(jnp.float32)).astype(jnp.bfloat16)
    logits = gate_logits.astype(jnp.float32)
    mixing = (logits / lax.optimization_barrier(jnp.sum(logits, axis=-1, keepdims=True))).astype(jnp.bfloat16)
    pair_count = TOK_DEV * TOP
    chosen = routes.reshape(SEQS, pair_count).astype(jnp.int32)
    live_rows = jnp.repeat(is_live, TOP).reshape(SEQS, pair_count)
    expert_hits = ((chosen[:, :, None] == jnp.arange(EXPERTS, dtype=jnp.int32)[None, None, :]) & live_rows[:, :, None]).astype(jnp.int32)
    slot_rank = lax.optimization_barrier(jnp.sum((jnp.cumsum(expert_hits, axis=1) - expert_hits) * expert_hits, axis=2))
    slot_span = SEQS * CAP
    dead_slot = EXPERTS * slot_span
    target = jnp.where(live_rows, chosen * slot_span + jnp.arange(SEQS, dtype=jnp.int32)[:, None] * CAP + slot_rank, dead_slot).astype(jnp.int32)
    row_token = jnp.repeat(token_ids, TOP).reshape(SEQS, pair_count)
    table = jnp.full((dead_slot + 1,), total_tokens, jnp.int32).at[target.reshape(-1)].set(row_token.reshape(-1))
    table = table[:dead_slot].reshape(EXPERTS, slot_span)
    padded = jnp.concatenate([hidden, jnp.zeros((1, D), jnp.bfloat16)], axis=0)

    def one_expert(expert_index):
        gathered = padded[table[expert_index]]
        gate_part = jnp.dot(gathered, w_gate[expert_index], preferred_element_type=jnp.float32)
        up_part = jnp.dot(gathered, w_up[expert_index], preferred_element_type=jnp.float32)
        active = (jax.nn.silu(gate_part) * up_part).astype(jnp.bfloat16)
        return jnp.dot(active, w_down[expert_index], preferred_element_type=jnp.float32).astype(jnp.bfloat16)
    expert_out = lax.map(one_expert, jnp.arange(EXPERTS, dtype=jnp.int32))
    flat_out = jnp.concatenate([expert_out.reshape(dead_slot, D), jnp.zeros((1, D), jnp.bfloat16)], axis=0)
    pair_slot = target.reshape(total_tokens, TOP)
    mixed = jnp.zeros((total_tokens, D), jnp.float32)
    for pick_index in range(TOP):
        mixed = mixed + mixing[:, pick_index].astype(jnp.float32)[:, None] * flat_out[pair_slot[:, pick_index]].astype(jnp.float32)
    moe_out = mixed.astype(jnp.bfloat16)
    head_rows = keys_raw.astype(jnp.float32).reshape(total_tokens, KV_HEADS, HEAD)
    normed = rms_scale(head_rows, k_gain.astype(jnp.float32))
    turned = rotate_keys(normed, position)
    key_rows = jnp.where(is_live[:, None, None], turned, 0.0).astype(jnp.bfloat16).reshape(total_tokens, KV_HEADS * HEAD)
    value_rows = jnp.where(is_live[:, None], values_raw, jnp.zeros_like(values_raw))
    stacked = jnp.stack([key_rows, value_rows], axis=1).reshape(SEQS * PAGES, PAGE, 2, KV_HEADS * HEAD)
    destination = (page_owner.astype(jnp.int32) * PAGES + page_slot.astype(jnp.int32)).reshape(-1)
    kv_cache = jnp.zeros_like(stacked).at[destination].set(stacked)
    return (moe_out, kv_cache)
```

```python
import math

import jax
import jax.numpy as jnp
from jax import lax
from jax.sharding import PartitionSpec as P

TOP = 8
CAP = 40
PAGE_PEER = 2
LANES = 128


def rms_scale(values, gain_row):
    mean_square = jnp.mean(values * values, axis=-1, keepdims=True)
    return values * lax.rsqrt(mean_square + 1e-06) * gain_row


def rotate_keys(key_block, position):
    half_size = key_block.shape[-1] // 2
    frequency = jnp.exp(
        jnp.arange(half_size, dtype=jnp.float32)
        * (-2.0 / key_block.shape[-1])
        * math.log(1000000.0)
    )
    angles = position.astype(jnp.float32)[:, None, None] * frequency
    cosine = jnp.cos(angles)
    sine_part = jnp.sin(angles)
    first_half = key_block[..., :half_size]
    second = key_block[..., half_size:]
    return jnp.concatenate(
        [first_half * cosine - second * sine_part, second * cosine + first_half * sine_part],
        axis=-1,
    )


class Ring:
    def __init__(self, count):
        order = list(range(0, count, 2)) + list(range(1, count, 2))[::-1]
        self.count = count
        self.up = [(order[i], order[(i + 1) % count]) for i in range(count)]
        self.down = [(b, a) for a, b in self.up]

    def clockwise(self, block):
        return lax.ppermute(block, "ep", self.up)

    def counter(self, block):
        return lax.ppermute(block, "ep", self.down)


def gather_ring(ring, block):
    half = ring.count // 2
    rows = block.shape[0] // 2
    behind, ahead = [block], [block]
    for _ in range(half - 1):
        behind.append(ring.clockwise(behind[-1]))
        ahead.append(ring.counter(ahead[-1]))
    far = jnp.concatenate(
        [ring.clockwise(behind[-1][:rows]), ring.counter(ahead[-1][rows:])], axis=0
    )
    return [block] + behind[1:] + ahead[1:] + [far]


def scatter_ring(ring, parts):
    half = ring.count // 2
    own, behind, ahead, far = parts[0], parts[1:half], parts[half : 2 * half - 1], parts[-1]
    rows = far.shape[0] // 2

    def merge(part, acc, low):
        if acc.shape[0] == part.shape[0]:
            return part + acc.astype(jnp.float32)
        pad = part.shape[0] - acc.shape[0]
        widths = ((0, pad), (0, 0)) if low else ((pad, 0), (0, 0))
        return part + jnp.pad(acc.astype(jnp.float32), widths)

    up = ring.clockwise(far[:rows].astype(jnp.bfloat16))
    down = ring.counter(far[rows:].astype(jnp.bfloat16))
    for step in range(half - 2, -1, -1):
        up = ring.clockwise(merge(ahead[step], up, True).astype(jnp.bfloat16))
        down = ring.counter(merge(behind[step], down, False).astype(jnp.bfloat16))
    return merge(merge(own, up, True), down, False)


def swap_section(block):
    return lax.ppermute(block, "section", [(0, 1), (1, 0)])


def kv_part(keys_raw, values_raw, k_gain, is_live, position, page_owner, page_slot):
    tok_rows, kv_width = keys_raw.shape
    head = k_gain.shape[0]
    pages = page_owner.shape[1]
    page = tok_rows // pages
    peer_count = lax.axis_size("ep")
    normed = rms_scale(
        keys_raw.astype(jnp.float32).reshape(tok_rows, kv_width // head, head),
        k_gain.astype(jnp.float32),
    )
    turned = rotate_keys(normed, position)
    key_rows = (
        jnp.where(is_live[:, None, None], turned, 0.0)
        .astype(jnp.bfloat16)
        .reshape(tok_rows, kv_width)
    )
    value_rows = jnp.where(is_live[:, None], values_raw, jnp.zeros_like(values_raw))
    page_rows = jnp.stack([key_rows, value_rows], axis=1).reshape(pages, page * 2 * kv_width)
    owners = page_owner.reshape(-1)
    same = (owners[:, None] == owners[None, :]) & (
        jnp.arange(pages)[None, :] < jnp.arange(pages)[:, None]
    )
    page_rank = jnp.sum(same.astype(jnp.int32), axis=1)
    lane_index = owners * PAGE_PEER + page_rank
    lane_ids = jnp.arange(peer_count * PAGE_PEER, dtype=jnp.int32)
    select = lane_ids[:, None] == lane_index[None, :]
    tagged = jnp.concatenate(
        [
            page_rows,
            jnp.broadcast_to(
                (page_slot.reshape(-1, 1) + 1).astype(jnp.bfloat16), (pages, LANES)
            ),
        ],
        axis=1,
    )
    sent = jnp.dot(
        select.astype(jnp.bfloat16), tagged, preferred_element_type=jnp.float32
    ).astype(jnp.bfloat16)
    sent = sent.reshape(peer_count, PAGE_PEER, tagged.shape[1])
    got = lax.all_to_all(sent, "ep", split_axis=0, concat_axis=0, tiled=True)
    got = got.reshape(peer_count * PAGE_PEER, tagged.shape[1])
    slots = got[:, -1].astype(jnp.int32) - 1
    placing = (jnp.arange(pages, dtype=jnp.int32)[:, None] == slots[None, :]).astype(jnp.bfloat16)
    cache = jnp.dot(placing, got[:, :-LANES], preferred_element_type=jnp.float32)
    return cache.astype(jnp.bfloat16).reshape(pages, page, 2, kv_width)


def shards(
    resid,
    norm_gain,
    gate_logits,
    routes,
    w_gate,
    w_up,
    w_down,
    keys_raw,
    values_raw,
    k_gain,
    lengths,
    page_owner,
    page_slot,
):
    tok_rows, model_width = resid.shape
    section_count = lax.axis_size("section")
    peer_count = lax.axis_size("ep")
    section = lax.axis_index("section")
    peer = lax.axis_index("ep")
    local_experts = w_gate.shape[0]
    experts = local_experts * peer_count
    col_width = model_width // section_count
    ring = Ring(peer_count)
    position = jnp.arange(tok_rows, dtype=jnp.int32)
    is_live = position < lengths[0]

    kv_cache = kv_part(keys_raw, values_raw, k_gain, is_live, position, page_owner, page_slot)

    hidden = rms_scale(resid.astype(jnp.float32), norm_gain.astype(jnp.float32)).astype(
        jnp.bfloat16
    )
    mixing = (gate_logits / jnp.sum(gate_logits, axis=-1, keepdims=True)).astype(jnp.bfloat16)
    chosen = (
        routes[:, :, None] == jnp.arange(experts, dtype=jnp.int32)[None, None, :]
    ) & is_live[:, None, None]
    hits = jnp.sum(chosen.astype(jnp.float32), axis=1)
    weights = jnp.sum(jnp.where(chosen, mixing.astype(jnp.float32)[:, :, None], 0.0), axis=1)
    earlier = (position[None, :] < position[:, None]).astype(jnp.bfloat16)
    rank = jnp.dot(earlier, hits.astype(jnp.bfloat16), preferred_element_type=jnp.float32)
    slot_of = jnp.where(hits > 0, rank, -1.0)
    table_width = -(-2 * experts // LANES) * LANES
    table = jnp.pad(
        jnp.concatenate([slot_of, weights], axis=1), ((0, 0), (0, table_width - 2 * experts))
    ).astype(jnp.bfloat16)
    payload = jnp.concatenate([hidden, table], axis=1)
    sec_rows = tok_rows // section_count
    mine = lax.dynamic_slice_in_dim(payload, section * sec_rows, sec_rows, axis=0)

    gathered = jnp.stack(gather_ring(ring, mine), axis=0)
    other = swap_section(gathered)
    both = jnp.concatenate([gathered, other], axis=1)
    inputs = both[:, :, :model_width]
    tables = both[:, :, model_width:]
    local = lax.dynamic_slice_in_dim(tables, peer * local_experts, local_experts, axis=2)
    slot_ids = jnp.arange(CAP, dtype=jnp.float32)
    match = local.astype(jnp.float32).transpose(0, 2, 1)[:, :, None, :] == slot_ids[:, None]
    place = match.astype(jnp.bfloat16).reshape(peer_count, local_experts * CAP, tok_rows)
    swapped = jnp.concatenate([both[:, sec_rows:, model_width:], both[:, :sec_rows, model_width:]], 1)
    true_tables = jnp.where(section == 0, tables, swapped)
    true_slot = lax.dynamic_slice_in_dim(true_tables, peer * local_experts, local_experts, axis=2)
    true_mix = lax.dynamic_slice_in_dim(
        true_tables, experts + peer * local_experts, local_experts, axis=2
    )
    combine = jnp.where(
        true_slot.astype(jnp.float32)[:, :, :, None] == slot_ids, true_mix[:, :, :, None], 0.0
    )
    combine = combine.astype(jnp.bfloat16).reshape(peer_count, tok_rows, local_experts * CAP)

    arrived = lax.dot_general(
        place, inputs, (((2,), (1,)), ((0,), (0,))), preferred_element_type=jnp.float32
    ).astype(jnp.bfloat16)
    arrived = arrived.reshape(peer_count, local_experts, CAP, model_width)
    gate_sum = jnp.einsum("sjcd,jdf->sjcf", arrived, w_gate, preferred_element_type=jnp.float32)
    up_sum = jnp.einsum("sjcd,jdf->sjcf", arrived, w_up, preferred_element_type=jnp.float32)
    active = (jax.nn.silu(gate_sum) * up_sum).astype(jnp.bfloat16)
    rows = jnp.einsum(
        "sjcf,jfd->sjcd", active, w_down, preferred_element_type=jnp.float32
    ).astype(jnp.bfloat16)
    rows = rows.reshape(peer_count, local_experts * CAP, model_width)

    def mix_columns(start):
        block = lax.dynamic_slice_in_dim(rows, start, col_width, axis=2)
        return lax.dot_general(
            combine, block, (((2,), (1,)), ((0,), (0,))), preferred_element_type=jnp.float32
        )

    given = mix_columns((1 - section) * col_width).astype(jnp.bfloat16)
    taken = swap_section(given)
    kept = mix_columns(section * col_width)
    total = kept + taken.astype(jnp.float32)
    moe_out = scatter_ring(ring, [total[i] for i in range(peer_count)]).astype(jnp.bfloat16)
    return (moe_out, kv_cache)


def solution(mesh):
    in_specs = (
        P(("groups", "ep"), None),
        P(),
        P(("groups", "ep"), None),
        P(("groups", "ep"), None),
        P("ep", None, "section"),
        P("ep", None, "section"),
        P("ep", "section", None),
        P(("groups", "ep"), "section"),
        P(("groups", "ep"), "section"),
        P(),
        P(("groups", "ep")),
        P(("groups", "ep"), None),
        P(("groups", "ep"), None),
    )
    out_specs = (P(("groups", "ep"), "section"), P(("groups", "ep"), None, None, "section"))
    return jax.shard_map(shards, mesh=mesh, in_specs=in_specs, out_specs=out_specs, check_vma=False)
```

```python
import functools
import math

import jax
import jax.numpy as jnp
from jax import lax
from jax.experimental import pallas as pl
from jax.experimental.pallas import tpu as pltpu
from jax.sharding import PartitionSpec as P

CAP = 40
PAGE_PEER = 2
LANES = 128
ROWS = 16
TILE = 128
CHUNKS = 2
VMEM_LIMIT = 60 * 1024 * 1024


def rms_scale(values, gain_row):
    mean_square = jnp.mean(values * values, axis=-1, keepdims=True)
    return values * lax.rsqrt(mean_square + 1e-06) * gain_row


def rotate_keys(key_block, position):
    half_size = key_block.shape[-1] // 2
    frequency = jnp.exp(
        jnp.arange(half_size, dtype=jnp.float32)
        * (-2.0 / key_block.shape[-1])
        * math.log(1000000.0)
    )
    angles = position.astype(jnp.float32)[:, None, None] * frequency
    cosine = jnp.cos(angles)
    sine_part = jnp.sin(angles)
    first_half = key_block[..., :half_size]
    second = key_block[..., half_size:]
    return jnp.concatenate(
        [first_half * cosine - second * sine_part, second * cosine + first_half * sine_part],
        axis=-1,
    )


class Ring:
    def __init__(self, count):
        order = list(range(0, count, 2)) + list(range(1, count, 2))[::-1]
        self.count = count
        self.half = count // 2
        self.up = [(order[i], order[(i + 1) % count]) for i in range(count)]
        self.down = [(b, a) for a, b in self.up]

    def clockwise(self, block):
        return lax.ppermute(block, "ep", self.up)

    def counter(self, block):
        return lax.ppermute(block, "ep", self.down)


def swap_section(block):
    return lax.ppermute(block, "section", [(0, 1), (1, 0)])


def prep_kernel(scalars, resid, gain, logits, routes, *outs, blocks):
    section = scalars[0]
    length = scalars[1]
    width = resid.shape[1]
    for chunk, out in enumerate(outs):
        for part in range(2):
            index = 2 * chunk + section
            block = index if part == 0 else blocks - 1 - index
            start = pl.multiple_of(block * ROWS, ROWS)
            values = resid[pl.ds(start, ROWS), :].astype(jnp.float32)
            mean_square = jnp.sum(values * values, axis=-1, keepdims=True) * (1.0 / width)
            scaled = values * lax.rsqrt(mean_square + 1e-06) * gain[...].astype(jnp.float32)
            out[part * ROWS : (part + 1) * ROWS, :width] = scaled.astype(jnp.bfloat16)
            weights = logits[pl.ds(start, ROWS), :]
            weights = weights / jnp.sum(weights, axis=-1, keepdims=True)
            weights = weights.astype(jnp.bfloat16).astype(jnp.float32)
            chosen = routes[pl.ds(start, ROWS), :]
            lanes = lax.broadcasted_iota(jnp.int32, (ROWS, LANES), 1)
            rows = start + lax.broadcasted_iota(jnp.int32, (ROWS, LANES), 0)
            table = jnp.zeros((ROWS, LANES), jnp.float32)
            for k in range(chosen.shape[1]):
                table = table + jnp.where(
                    lanes == chosen[:, k : k + 1], weights[:, k : k + 1], 0.0
                )
            table = jnp.where(rows < length, table, 0.0)
            out[part * ROWS : (part + 1) * ROWS, width:] = table.astype(jnp.bfloat16)


def prep(section, length, resid, gain, logits, routes):
    tok_rows, width = resid.shape
    rows = 2 * ROWS
    whole = pl.BlockSpec(memory_space=pltpu.VMEM)
    return pl.pallas_call(
        functools.partial(prep_kernel, blocks=tok_rows // ROWS),
        out_shape=[jax.ShapeDtypeStruct((rows, width + LANES), jnp.bfloat16)] * CHUNKS,
        in_specs=[pl.BlockSpec(memory_space=pltpu.SMEM)] + [whole] * 4,
        out_specs=[whole] * CHUNKS,
        name="prep",
    )(jnp.stack([section, length]).astype(jnp.int32), resid, gain.reshape(1, width), logits, routes)


def gate_kernel(peer, *refs, count, tokens, width, local):
    blocks = refs[:count]
    w_gate, w_up, active, slot_out, mix_out, total_out, hold, slot_t, sems = refs[count:]
    expert = pl.program_id(0)

    @pl.when(expert == 0)
    def _():
        copies = []
        start = 0
        for i, block in enumerate(blocks):
            rows = block.shape[0]
            copy = pltpu.make_async_copy(block, hold.at[pl.ds(start, rows), :], sems.at[i])
            copy.start()
            copies.append(copy)
            start += rows
        for copy in copies:
            copy.wait()
        lane_in = lax.broadcasted_iota(jnp.int32, (LANES, LANES), 0)
        lane_out = lax.broadcasted_iota(jnp.int32, (LANES, LANES), 1)
        pick = ((lane_in == peer[0] * local + lane_out) & (lane_out < local)).astype(jnp.bfloat16)
        earlier = (lane_out < lane_in).astype(jnp.bfloat16)
        carry = jnp.zeros((1, LANES), jnp.float32)
        for b in range(tokens // LANES):
            span = slice(b * LANES, (b + 1) * LANES)
            mix = jnp.dot(hold[span, width:], pick, preferred_element_type=jnp.float32)
            hit = (mix > 0.0).astype(jnp.float32)
            rank = carry + jnp.dot(
                earlier, hit.astype(jnp.bfloat16), preferred_element_type=jnp.float32
            )
            slot = jnp.where(mix > 0.0, rank, -1.0)
            carry = carry + jnp.sum(hit, axis=0, keepdims=True)
            slot_out[span, :] = slot
            mix_out[span, :] = mix
            slot_t[:, span] = slot.T[: slot_t.shape[0], :]
        total_out[...] = jnp.broadcast_to(carry, total_out.shape)

    lane = lax.broadcasted_iota(jnp.int32, total_out.shape, 1)
    found = jnp.max(jnp.where(lane == expert, total_out[...], 0.0)).astype(jnp.int32)
    slots = slot_t[pl.ds(expert, 1), :]
    step = min(width, 1024)

    def tile(t, _):
        row = lax.broadcasted_iota(jnp.int32, (TILE, tokens), 0) + t * TILE
        select = (slots == row.astype(jnp.float32)).astype(jnp.bfloat16)
        gate = jnp.zeros((TILE, w_gate.shape[2]), jnp.float32)
        up = jnp.zeros((TILE, w_gate.shape[2]), jnp.float32)
        for k in range(width // step):
            span = slice(k * step, (k + 1) * step)
            x = jnp.dot(select, hold[:, span], preferred_element_type=jnp.float32)
            x = x.astype(jnp.bfloat16)
            gate = gate + jnp.dot(x, w_gate[0, span, :], preferred_element_type=jnp.float32)
            up = up + jnp.dot(x, w_up[0, span, :], preferred_element_type=jnp.float32)
        value = gate / (1.0 + jnp.exp(-gate)) * up
        active[0, pl.ds(pl.multiple_of(t * TILE, TILE), TILE), :] = value.astype(jnp.bfloat16)
        return 0

    lax.fori_loop(0, (found + TILE - 1) // TILE, tile, 0)


def gate_up(peer, blocks, w_gate, w_up, capacity):
    local, width, units = w_gate.shape
    tokens = sum(block.shape[0] for block in blocks)
    weight = pl.BlockSpec((1, width, units), lambda e, *_: (e, 0, 0))
    keep = lambda *shape: pl.BlockSpec(shape, lambda e, *_: (0,) * len(shape))
    sub = max(8, local)
    return pl.pallas_call(
        functools.partial(
            gate_kernel, count=len(blocks), tokens=tokens, width=width, local=local
        ),
        grid_spec=pltpu.PrefetchScalarGridSpec(
            num_scalar_prefetch=1,
            grid=(local,),
            in_specs=[pl.BlockSpec(memory_space=pl.ANY)] * len(blocks) + [weight, weight],
            out_specs=[
                pl.BlockSpec((1, capacity, units), lambda e, *_: (e, 0, 0)),
                keep(tokens, LANES),
                keep(tokens, LANES),
                keep(8, LANES),
            ],
            scratch_shapes=[
                pltpu.VMEM((tokens, width + LANES), jnp.bfloat16),
                pltpu.VMEM((sub, tokens), jnp.float32),
                pltpu.SemaphoreType.DMA((len(blocks),)),
            ],
        ),
        out_shape=[
            jax.ShapeDtypeStruct((local, capacity, units), jnp.bfloat16),
            jax.ShapeDtypeStruct((tokens, LANES), jnp.float32),
            jax.ShapeDtypeStruct((tokens, LANES), jnp.float32),
            jax.ShapeDtypeStruct((8, LANES), jnp.float32),
        ],
        compiler_params=pltpu.CompilerParams(
            dimension_semantics=("arbitrary",), vmem_limit_bytes=VMEM_LIMIT
        ),
        cost_estimate=pl.CostEstimate(
            flops=8_000_000_000, bytes_accessed=4 * local * width * units, transcendentals=0
        ),
        name="gate_up",
    )(peer, *blocks, w_gate, w_up)


def down_kernel(offset, active, slots, mixes, totals, w_down, out, spread, held, total, *, levels):
    local = active.shape[0]
    tokens = slots.shape[0]
    lane = lax.broadcasted_iota(jnp.int32, totals.shape, 1)
    most = jnp.max(jnp.where(lane < local, totals[...], 0.0)).astype(jnp.int32)
    used = (most + TILE - 1) // TILE

    @pl.when(pl.program_id(0) == 0)
    def _():
        def build(level, _):
            column = lax.broadcasted_iota(jnp.int32, (tokens, TILE), 1) + level * TILE
            column = column.astype(jnp.float32)
            for e in range(local):
                hit = slots[:, e : e + 1] == column
                spread[level, :, e * TILE : (e + 1) * TILE] = jnp.where(
                    hit, mixes[:, e : e + 1], 0.0
                ).astype(jnp.bfloat16)
            return 0

        lax.fori_loop(0, used, build, 0)

    total[...] = jnp.zeros_like(total)

    def add(level, _):
        for e in range(local):
            found = jnp.max(jnp.where(lane == e, totals[...], 0.0)).astype(jnp.int32)
            rows = slice(e * TILE, (e + 1) * TILE)

            @pl.when(found > level * TILE)
            def _():
                start = pl.multiple_of(level * TILE, TILE)
                held[rows, :] = jnp.dot(
                    active[e, pl.ds(start, TILE), :],
                    w_down[e],
                    preferred_element_type=jnp.float32,
                ).astype(jnp.bfloat16)

            @pl.when(found <= level * TILE)
            def _():
                held[rows, :] = jnp.zeros((TILE, held.shape[1]), held.dtype)

        total[...] += jnp.dot(spread[level], held[...], preferred_element_type=jnp.float32)
        return 0

    lax.fori_loop(0, used, add, 0)
    out[...] = total[...].astype(out.dtype)


def down_mix(half, active, slots, mixes, totals, w_down, columns, dtype, step=512):
    local, capacity, units = active.shape
    tokens = slots.shape[0]
    steps = columns // step
    levels = capacity // TILE
    keep = lambda *shape: pl.BlockSpec(shape, lambda n, *_: (0,) * len(shape))
    return pl.pallas_call(
        functools.partial(down_kernel, levels=levels),
        grid_spec=pltpu.PrefetchScalarGridSpec(
            num_scalar_prefetch=1,
            grid=(steps,),
            in_specs=[
                keep(local, capacity, units),
                keep(tokens, LANES),
                keep(tokens, LANES),
                keep(8, LANES),
                pl.BlockSpec((local, units, step), lambda n, h: (0, 0, h[0] * steps + n)),
            ],
            out_specs=pl.BlockSpec((tokens, step), lambda n, h: (0, n)),
            scratch_shapes=[
                pltpu.VMEM((levels, tokens, local * TILE), jnp.bfloat16),
                pltpu.VMEM((local * TILE, step), jnp.bfloat16),
                pltpu.VMEM((tokens, step), jnp.float32),
            ],
        ),
        out_shape=jax.ShapeDtypeStruct((tokens, columns), dtype),
        compiler_params=pltpu.CompilerParams(
            dimension_semantics=("arbitrary",), vmem_limit_bytes=VMEM_LIMIT
        ),
        cost_estimate=pl.CostEstimate(
            flops=3_000_000_000, bytes_accessed=2 * local * units * columns, transcendentals=0
        ),
        name="down_mix",
    )(half, active, slots, mixes, totals, w_down)


def gather_ring(ring, block):
    rows = block.shape[0] // 2
    behind, ahead = [block], [block]
    for _ in range(ring.half - 1):
        behind.append(ring.clockwise(behind[-1]))
        ahead.append(ring.counter(ahead[-1]))
    far = [ring.clockwise(behind[-1][:rows]), ring.counter(ahead[-1][rows:])]
    return [block] + behind[1:] + ahead[1:] + far


def scatter_ring(ring, part):
    half = ring.half

    def merge(index, up, down):
        sides = []
        for side in range(2):
            value = part(index, side)
            for acc in (up, down):
                if acc is not None and side in acc:
                    value = value + acc[side].astype(jnp.float32)
            sides.append(value)
        return sides

    def send(move, sides, which):
        block = jnp.concatenate([sides[s].astype(jnp.bfloat16) for s in which], axis=0)
        block = move(block)
        rows = block.shape[0] // len(which)
        return {s: block[i * rows : (i + 1) * rows] for i, s in enumerate(which)}

    far = 2 * half - 1
    up = send(ring.clockwise, {0: part(far, 0)}, [0])
    down = send(ring.counter, {1: part(far, 1)}, [1])
    for step in range(half - 1, 0, -1):
        up = send(ring.clockwise, merge(half - 1 + step, up, None), [0, 1])
        down = send(ring.counter, merge(step, None, down), [0, 1])
    return [side.astype(jnp.bfloat16) for side in merge(0, up, down)]


def kv_part(keys_raw, values_raw, k_gain, is_live, position, page_owner, page_slot):
    tok_rows, kv_width = keys_raw.shape
    head = k_gain.shape[0]
    pages = page_owner.shape[1]
    page = tok_rows // pages
    peer_count = lax.axis_size("ep")
    normed = rms_scale(
        keys_raw.astype(jnp.float32).reshape(tok_rows, kv_width // head, head),
        k_gain.astype(jnp.float32),
    )
    turned = rotate_keys(normed, position)
    key_rows = (
        jnp.where(is_live[:, None, None], turned, 0.0)
        .astype(jnp.bfloat16)
        .reshape(tok_rows, kv_width)
    )
    value_rows = jnp.where(is_live[:, None], values_raw, jnp.zeros_like(values_raw))
    page_rows = jnp.stack([key_rows, value_rows], axis=1).reshape(pages, page * 2 * kv_width)
    owners = page_owner.reshape(-1)
    same = (owners[:, None] == owners[None, :]) & (
        jnp.arange(pages)[None, :] < jnp.arange(pages)[:, None]
    )
    page_rank = jnp.sum(same.astype(jnp.int32), axis=1)
    lane_index = owners * PAGE_PEER + page_rank
    lane_ids = jnp.arange(peer_count * PAGE_PEER, dtype=jnp.int32)
    select = lane_ids[:, None] == lane_index[None, :]
    tagged = jnp.concatenate(
        [
            page_rows,
            jnp.broadcast_to(
                (page_slot.reshape(-1, 1) + 1).astype(jnp.bfloat16), (pages, LANES)
            ),
        ],
        axis=1,
    )
    sent = jnp.dot(
        select.astype(jnp.bfloat16), tagged, preferred_element_type=jnp.float32
    ).astype(jnp.bfloat16)
    sent = sent.reshape(peer_count, PAGE_PEER, tagged.shape[1])
    got = lax.all_to_all(sent, "ep", split_axis=0, concat_axis=0, tiled=True)
    got = got.reshape(peer_count * PAGE_PEER, tagged.shape[1])
    slots = got[:, -1].astype(jnp.int32) - 1
    placing = (jnp.arange(pages, dtype=jnp.int32)[:, None] == slots[None, :]).astype(jnp.bfloat16)
    cache = jnp.dot(placing, got[:, :-LANES], preferred_element_type=jnp.float32)
    return cache.astype(jnp.bfloat16).reshape(pages, page, 2, kv_width)


def shards(
    resid,
    norm_gain,
    gate_logits,
    routes,
    w_gate,
    w_up,
    w_down,
    keys_raw,
    values_raw,
    k_gain,
    lengths,
    page_owner,
    page_slot,
):
    tok_rows, model_width = resid.shape
    section_count = lax.axis_size("section")
    peer_count = lax.axis_size("ep")
    section = lax.axis_index("section")
    peer = lax.axis_index("ep").reshape(1).astype(jnp.int32)
    col_width = model_width // section_count
    ring = Ring(peer_count)
    position = jnp.arange(tok_rows, dtype=jnp.int32)
    is_live = position < lengths[0]

    kv_cache = kv_part(keys_raw, values_raw, k_gain, is_live, position, page_owner, page_slot)

    chunk_rows = tok_rows // CHUNKS
    tokens = peer_count * chunk_rows
    capacity = -(-peer_count * min(CAP, chunk_rows) // TILE) * TILE
    payloads = prep(section, lengths[0], resid, norm_gain, gate_logits, routes)
    gathered = [gather_ring(ring, payload) for payload in payloads]
    halves = []
    mine = section.reshape(1).astype(jnp.int32)
    for chunk in range(CHUNKS):
        own = gathered[chunk]
        other = [swap_section(block) for block in own]
        active, slots, mixes, totals = gate_up(peer, own + other, w_gate, w_up, capacity)
        given = down_mix(1 - mine, active, slots, mixes, totals, w_down, col_width, jnp.bfloat16)
        taken = swap_section(given)
        kept = down_mix(mine, active, slots, mixes, totals, w_down, col_width, jnp.float32)
        rows = tokens // (2 * peer_count)

        def part(index, side, kept=kept, taken=taken, rows=rows):
            here = (side * peer_count + index) * rows
            there = ((1 - side) * peer_count + index) * rows
            return kept[here : here + rows] + taken[there : there + rows].astype(jnp.float32)

        halves.append(scatter_ring(ring, part))

    blocks = [None] * (tok_rows // ROWS)
    first = section == 0
    for chunk, (own, other) in enumerate(halves):
        for core in range(2):
            rows = jnp.where(first, own, other) if core == 0 else jnp.where(first, other, own)
            index = 2 * chunk + core
            blocks[index] = rows[:ROWS]
            blocks[len(blocks) - 1 - index] = rows[ROWS:]
    return (jnp.concatenate(blocks, axis=0), kv_cache)


def solution(mesh):
    in_specs = (
        P(("groups", "ep"), None),
        P(),
        P(("groups", "ep"), None),
        P(("groups", "ep"), None),
        P("ep", None, "section"),
        P("ep", None, "section"),
        P("ep", "section", None),
        P(("groups", "ep"), "section"),
        P(("groups", "ep"), "section"),
        P(),
        P(("groups", "ep")),
        P(("groups", "ep"), None),
        P(("groups", "ep"), None),
    )
    out_specs = (P(("groups", "ep"), "section"), P(("groups", "ep"), None, None, "section"))
    return jax.shard_map(shards, mesh=mesh, in_specs=in_specs, out_specs=out_specs, check_vma=False)
```

```python
import functools
import math

import jax
import jax.numpy as jnp
from jax import lax
from jax.experimental import pallas as pl
from jax.experimental.pallas import tpu as pltpu
from jax.sharding import PartitionSpec as P

CAP = 40
PAGE_PEER = 2
LANES = 128
TILE = 160
PARTS = 2
VMEM_LIMIT = 60 * 1024 * 1024


def rms_scale(values, gain_row):
    mean_square = jnp.mean(values * values, axis=-1, keepdims=True)
    return values * lax.rsqrt(mean_square + 1e-06) * gain_row


def rotate_keys(key_block, position):
    half_size = key_block.shape[-1] // 2
    frequency = jnp.exp(
        jnp.arange(half_size, dtype=jnp.float32)
        * (-2.0 / key_block.shape[-1])
        * math.log(1000000.0)
    )
    angles = position.astype(jnp.float32)[:, None, None] * frequency
    cosine = jnp.cos(angles)
    sine_part = jnp.sin(angles)
    first_half = key_block[..., :half_size]
    second = key_block[..., half_size:]
    return jnp.concatenate(
        [first_half * cosine - second * sine_part, second * cosine + first_half * sine_part],
        axis=-1,
    )


class Ring:
    def __init__(self, count):
        order = list(range(0, count, 2)) + list(range(1, count, 2))[::-1]
        self.count = count
        self.half = count // 2
        self.up = [(order[i], order[(i + 1) % count]) for i in range(count)]
        self.down = [(b, a) for a, b in self.up]

    def clockwise(self, block):
        return lax.ppermute(block, "ep", self.up)

    def counter(self, block):
        return lax.ppermute(block, "ep", self.down)


def swap_section(block):
    return lax.ppermute(block, "section", [(0, 1), (1, 0)])


def prep_kernel(scalars, resid, gain, logits, routes, out):
    rows, width = out.shape[0], resid.shape[1]
    start = pl.multiple_of(scalars[0] * rows, rows)
    values = resid[pl.ds(start, rows), :].astype(jnp.float32)
    mean_square = jnp.sum(values * values, axis=-1, keepdims=True) * (1.0 / width)
    scaled = values * lax.rsqrt(mean_square + 1e-06) * gain[...].astype(jnp.float32)
    out[:, :width] = scaled.astype(jnp.bfloat16)
    weights = logits[pl.ds(start, rows), :]
    weights = weights / jnp.sum(weights, axis=-1, keepdims=True)
    weights = weights.astype(jnp.bfloat16).astype(jnp.float32)
    chosen = routes[pl.ds(start, rows), :]
    lanes = lax.broadcasted_iota(jnp.int32, (rows, LANES), 1)
    position = start + lax.broadcasted_iota(jnp.int32, (rows, LANES), 0)
    table = jnp.zeros((rows, LANES), jnp.float32)
    for k in range(chosen.shape[1]):
        table = table + jnp.where(lanes == chosen[:, k : k + 1], weights[:, k : k + 1], 0.0)
    out[:, width:] = jnp.where(position < scalars[1], table, 0.0).astype(jnp.bfloat16)


def prep(section, length, resid, gain, logits, routes):
    tok_rows, width = resid.shape
    whole = pl.BlockSpec(memory_space=pltpu.VMEM)
    return pl.pallas_call(
        prep_kernel,
        out_shape=jax.ShapeDtypeStruct((tok_rows // 2, width + LANES), jnp.bfloat16),
        in_specs=[pl.BlockSpec(memory_space=pltpu.SMEM)] + [whole] * 4,
        out_specs=whole,
        name="prep",
    )(jnp.stack([section, length]).astype(jnp.int32), resid, gain.reshape(1, width), logits, routes)


def gate_kernel(peer, *refs, count, tokens, width, local, levels):
    blocks = refs[:count]
    w_gate, w_up, active, spread = refs[count : count + 4]
    hold, gates, ups, picked, slot_t, block_sems, weight_sems = refs[count + 4 :]
    copies = []
    start = 0
    for i, block in enumerate(blocks):
        rows = block.shape[0]
        copy = pltpu.make_async_copy(block, hold.at[pl.ds(start, rows), :], block_sems.at[i])
        copy.start()
        copies.append(copy)
        start += rows

    def weights(e):
        return (
            pltpu.make_async_copy(w_gate.at[e], gates.at[e], weight_sems.at[0, e]),
            pltpu.make_async_copy(w_up.at[e], ups.at[e], weight_sems.at[1, e]),
        )

    for copy in weights(0):
        copy.start()
    for copy in copies:
        copy.wait()
    if local > 1:
        for copy in weights(1):
            copy.start()

    lane_in = lax.broadcasted_iota(jnp.int32, (LANES, LANES), 0)
    lane_out = lax.broadcasted_iota(jnp.int32, (LANES, LANES), 1)
    pick = ((lane_in == peer[0] * local + lane_out) & (lane_out < local)).astype(jnp.bfloat16)
    earlier = (lane_out < lane_in).astype(jnp.bfloat16)
    carry = jnp.zeros((1, LANES), jnp.float32)
    capacity = levels * TILE
    column = lax.broadcasted_iota(jnp.int32, (LANES, capacity), 1).astype(jnp.float32)
    for b in range(tokens // LANES):
        span = slice(b * LANES, (b + 1) * LANES)
        mix = jnp.dot(hold[span, width:], pick, preferred_element_type=jnp.float32)
        hit = (mix > 0.0).astype(jnp.float32)
        rank = jnp.dot(earlier, hit.astype(jnp.bfloat16), preferred_element_type=jnp.float32)
        slot = jnp.where(mix > 0.0, rank + carry, -1.0)
        carry = carry + jnp.sum(hit, axis=0, keepdims=True)
        slot_t[:, span] = slot.T[: slot_t.shape[0], :]
        pieces = [
            jnp.where(slot[:, e : e + 1] == column, mix[:, e : e + 1], 0.0) for e in range(local)
        ]
        spread[span, :] = jnp.concatenate(pieces, axis=1).astype(jnp.bfloat16)

    def tile(level, e):
        row = lax.broadcasted_iota(jnp.int32, (TILE, tokens), 0) + level * TILE
        select = (slot_t[pl.ds(e, 1), :] == row.astype(jnp.float32)).astype(jnp.bfloat16)
        step = min(width, 1024)
        for k in range(width // step):
            span = slice(k * step, (k + 1) * step)
            picked[:, span] = jnp.dot(
                select, hold[:, span], preferred_element_type=jnp.float32
            ).astype(jnp.bfloat16)
        gate = jnp.dot(picked[...], gates[e], preferred_element_type=jnp.float32)
        up = jnp.dot(picked[...], ups[e], preferred_element_type=jnp.float32)
        value = gate / (1.0 + jnp.exp(-gate)) * up
        active[e, pl.ds(pl.multiple_of(level * TILE, 32), TILE), :] = value.astype(jnp.bfloat16)

    def expert(e, _):
        for copy in weights(e):
            copy.wait()

        @pl.when(e + 2 < local)
        def _():
            for copy in weights(e + 2):
                copy.start()

        if levels == 1:
            tile(0, e)
        else:
            lax.fori_loop(0, levels, lambda level, _: (tile(level, e), 0)[1], 0)
        return 0

    lax.fori_loop(0, local, expert, 0)


def gate_up(peer, blocks, w_gate, w_up, levels):
    local, width, units = w_gate.shape
    tokens = sum(block.shape[0] for block in blocks)
    hbm = pl.BlockSpec(memory_space=pl.ANY)
    vmem = pl.BlockSpec(memory_space=pltpu.VMEM)
    smem = pl.BlockSpec(memory_space=pltpu.SMEM)
    return pl.pallas_call(
        functools.partial(
            gate_kernel,
            count=len(blocks),
            tokens=tokens,
            width=width,
            local=local,
            levels=levels,
        ),
        in_specs=[smem] + [hbm] * (len(blocks) + 2),
        out_specs=[vmem, vmem],
        scratch_shapes=[
            pltpu.VMEM((tokens, width + LANES), jnp.bfloat16),
            pltpu.VMEM((local, width, units), jnp.bfloat16),
            pltpu.VMEM((local, width, units), jnp.bfloat16),
            pltpu.VMEM((TILE, width), jnp.bfloat16),
            pltpu.VMEM((max(8, local), tokens), jnp.float32),
            pltpu.SemaphoreType.DMA((len(blocks),)),
            pltpu.SemaphoreType.DMA((2, local)),
        ],
        out_shape=[
            jax.ShapeDtypeStruct((local, levels * TILE, units), jnp.bfloat16),
            jax.ShapeDtypeStruct((tokens, local * levels * TILE), jnp.bfloat16),
        ],
        compiler_params=pltpu.CompilerParams(vmem_limit_bytes=VMEM_LIMIT),
        cost_estimate=pl.CostEstimate(
            flops=8_000_000_000, bytes_accessed=4 * local * width * units, transcendentals=0
        ),
        name="gate_up",
    )(peer, *blocks, w_gate, w_up)


def down_kernel(half, active, spread, w_down, *rest):
    out, held = rest[-2:]
    local, capacity, _ = active.shape
    for e in range(local):
        held[e * capacity : (e + 1) * capacity, :] = jnp.dot(
            active[e], w_down[e], preferred_element_type=jnp.float32
        ).astype(jnp.bfloat16)
    out[...] = jnp.dot(spread[...], held[...], preferred_element_type=jnp.float32).astype(out.dtype)


def down_mix(half, active, spread, w_down, columns, dtype, after=(), step=512):
    local, capacity, units = active.shape
    tokens = spread.shape[0]
    steps = columns // step
    keep = lambda *shape: pl.BlockSpec(shape, lambda n, *_: (0,) * len(shape))
    return pl.pallas_call(
        down_kernel,
        grid_spec=pltpu.PrefetchScalarGridSpec(
            num_scalar_prefetch=1,
            grid=(steps,),
            in_specs=[
                keep(local, capacity, units),
                keep(tokens, local * capacity),
                pl.BlockSpec((local, units, step), lambda n, h: (0, 0, h[0] * steps + n)),
            ]
            + [pl.BlockSpec(memory_space=pl.ANY)] * len(after),
            out_specs=pl.BlockSpec((tokens, step), lambda n, h: (0, n)),
            scratch_shapes=[pltpu.VMEM((local * capacity, step), jnp.bfloat16)],
        ),
        out_shape=jax.ShapeDtypeStruct((tokens, columns), dtype),
        compiler_params=pltpu.CompilerParams(
            dimension_semantics=("arbitrary",), vmem_limit_bytes=VMEM_LIMIT
        ),
        cost_estimate=pl.CostEstimate(
            flops=3_000_000_000, bytes_accessed=2 * local * units * columns, transcendentals=0
        ),
        name="down_mix",
    )(half, active, spread, w_down, *after)


def gather_ring(ring, block):
    rows = block.shape[0] // 2
    behind, ahead = [block], [block]
    found = [[block]]
    for _ in range(ring.half - 1):
        behind.append(ring.clockwise(behind[-1]))
        ahead.append(ring.counter(ahead[-1]))
        found += [[behind[-1]], [ahead[-1]]]
    found.append([ring.clockwise(behind[-1][:rows]), ring.counter(ahead[-1][rows:])])
    return found


def scatter_ring(ring, part):
    def merge(index, up, down):
        sides = []
        for side in range(2):
            value = part(index, side)
            for acc in (up, down):
                if acc is not None and side in acc:
                    value = value + acc[side].astype(jnp.float32)
            sides.append(value)
        return sides

    def send(move, sides, which):
        block = jnp.concatenate([sides[s].astype(jnp.bfloat16) for s in which], axis=0)
        block = move(block)
        rows = block.shape[0] // len(which)
        return {s: block[i * rows : (i + 1) * rows] for i, s in enumerate(which)}

    far = ring.count - 1
    up = send(ring.clockwise, {0: part(far, 0)}, [0])
    down = send(ring.counter, {1: part(far, 1)}, [1])
    for step in range(ring.half - 1, 0, -1):
        up = send(ring.clockwise, merge(2 * step, up, None), [0, 1])
        down = send(ring.counter, merge(2 * step - 1, None, down), [0, 1])
    return [side.astype(jnp.bfloat16) for side in merge(0, up, down)]


def kv_part(keys_raw, values_raw, k_gain, is_live, position, page_owner, page_slot):
    tok_rows, kv_width = keys_raw.shape
    head = k_gain.shape[0]
    pages = page_owner.shape[1]
    page = tok_rows // pages
    peer_count = lax.axis_size("ep")
    normed = rms_scale(
        keys_raw.astype(jnp.float32).reshape(tok_rows, kv_width // head, head),
        k_gain.astype(jnp.float32),
    )
    turned = rotate_keys(normed, position)
    key_rows = (
        jnp.where(is_live[:, None, None], turned, 0.0)
        .astype(jnp.bfloat16)
        .reshape(tok_rows, kv_width)
    )
    value_rows = jnp.where(is_live[:, None], values_raw, jnp.zeros_like(values_raw))
    page_rows = jnp.stack([key_rows, value_rows], axis=1).reshape(pages, page * 2 * kv_width)
    owners = page_owner.reshape(-1)
    same = (owners[:, None] == owners[None, :]) & (
        jnp.arange(pages)[None, :] < jnp.arange(pages)[:, None]
    )
    page_rank = jnp.sum(same.astype(jnp.int32), axis=1)
    lane_index = owners * PAGE_PEER + page_rank
    lane_ids = jnp.arange(peer_count * PAGE_PEER, dtype=jnp.int32)
    select = lane_ids[:, None] == lane_index[None, :]
    tagged = jnp.concatenate(
        [
            page_rows,
            jnp.broadcast_to(
                (page_slot.reshape(-1, 1) + 1).astype(jnp.bfloat16), (pages, LANES)
            ),
        ],
        axis=1,
    )
    sent = jnp.dot(
        select.astype(jnp.bfloat16), tagged, preferred_element_type=jnp.float32
    ).astype(jnp.bfloat16)
    sent = sent.reshape(peer_count, PAGE_PEER, tagged.shape[1])
    got = lax.all_to_all(sent, "ep", split_axis=0, concat_axis=0, tiled=True)
    got = got.reshape(peer_count * PAGE_PEER, tagged.shape[1])
    slots = got[:, -1].astype(jnp.int32) - 1
    placing = (jnp.arange(pages, dtype=jnp.int32)[:, None] == slots[None, :]).astype(jnp.bfloat16)
    cache = jnp.dot(placing, got[:, :-LANES], preferred_element_type=jnp.float32)
    return cache.astype(jnp.bfloat16).reshape(pages, page, 2, kv_width)


def shards(
    resid,
    norm_gain,
    gate_logits,
    routes,
    w_gate,
    w_up,
    w_down,
    keys_raw,
    values_raw,
    k_gain,
    lengths,
    page_owner,
    page_slot,
):
    tok_rows, model_width = resid.shape
    section_count = lax.axis_size("section")
    peer_count = lax.axis_size("ep")
    section = lax.axis_index("section")
    peer = lax.axis_index("ep").reshape(1).astype(jnp.int32)
    col_width = model_width // section_count
    ring = Ring(peer_count)
    position = jnp.arange(tok_rows, dtype=jnp.int32)
    is_live = position < lengths[0]

    kv_cache = kv_part(keys_raw, values_raw, k_gain, is_live, position, page_owner, page_slot)

    mine = section.reshape(1).astype(jnp.int32)
    near_count = peer_count // 2
    levels = -(-near_count * CAP // TILE)
    rows = tok_rows // section_count
    payload = prep(section, lengths[0], resid, norm_gain, gate_logits, routes)
    found = gather_ring(ring, payload)
    swapped = [[swap_section(piece) for piece in pieces] for pieces in found]
    groups = []
    for span in (slice(0, near_count), slice(near_count, peer_count)):
        blocks = [piece for pieces in found[span] + swapped[span] for piece in pieces]
        groups.append(gate_up(peer, blocks, w_gate, w_up, levels))
    sums = [None, None]
    after = ()
    for group in (1, 0):
        active, spread = groups[group]
        given = down_mix(1 - mine, active, spread, w_down, col_width, jnp.bfloat16, after)
        taken = swap_section(given)
        kept = down_mix(mine, active, spread, w_down, col_width, jnp.float32, (given,))
        sums[group] = (kept, taken)
        after = (kept,)

    pieces = []
    width = col_width // PARTS
    for column in range(PARTS):
        cols = slice(column * width, (column + 1) * width)

        def part(index, side, cols=cols):
            kept, taken = sums[index // near_count]
            place = index % near_count
            here = (side * near_count + place) * rows
            there = ((1 - side) * near_count + place) * rows
            return kept[here : here + rows, cols] + taken[there : there + rows, cols].astype(
                jnp.float32
            )

        own, other = scatter_ring(ring, part)
        first = section == 0
        pieces.append(
            jnp.concatenate(
                [jnp.where(first, own, other), jnp.where(first, other, own)], axis=0
            )
        )
    return (jnp.concatenate(pieces, axis=1), kv_cache)


def solution(mesh):
    in_specs = (
        P(("groups", "ep"), None),
        P(),
        P(("groups", "ep"), None),
        P(("groups", "ep"), None),
        P("ep", None, "section"),
        P("ep", None, "section"),
        P("ep", "section", None),
        P(("groups", "ep"), "section"),
        P(("groups", "ep"), "section"),
        P(),
        P(("groups", "ep")),
        P(("groups", "ep"), None),
        P(("groups", "ep"), None),
    )
    out_specs = (P(("groups", "ep"), "section"), P(("groups", "ep"), None, None, "section"))
    return jax.shard_map(shards, mesh=mesh, in_specs=in_specs, out_specs=out_specs, check_vma=False)
```

```python
import functools
import math

import jax
import jax.numpy as jnp
from jax import lax
from jax.experimental import pallas as pl
from jax.experimental.pallas import tpu as pltpu
from jax.sharding import PartitionSpec as P


CAP = 40
PAGE_PEER = 2
LANES = 128
TILE = 160
PARTS = 2
GATE_LIMIT = 48 * 1024 * 1024
DOWN_LIMIT = 24 * 1024 * 1024
SMALL_LIMIT = 12 * 1024 * 1024


def rms_scale(values, gain_row):
    mean_square = jnp.mean(values * values, axis=-1, keepdims=True)
    return values * lax.rsqrt(mean_square + 1e-06) * gain_row


def rotate_keys(key_block, position):
    half_size = key_block.shape[-1] // 2
    frequency = jnp.exp(
        jnp.arange(half_size, dtype=jnp.float32)
        * (-2.0 / key_block.shape[-1])
        * math.log(1000000.0)
    )
    angles = position.astype(jnp.float32)[:, None, None] * frequency
    cosine = jnp.cos(angles)
    sine_part = jnp.sin(angles)
    first_half = key_block[..., :half_size]
    second = key_block[..., half_size:]
    return jnp.concatenate(
        [first_half * cosine - second * sine_part, second * cosine + first_half * sine_part],
        axis=-1,
    )


class Ring:
    def __init__(self, count):
        order = list(range(0, count, 2)) + list(range(1, count, 2))[::-1]
        self.count = count
        self.half = count // 2
        self.up = [(order[i], order[(i + 1) % count]) for i in range(count)]
        self.down = [(b, a) for a, b in self.up]

    def clockwise(self, block):
        return lax.ppermute(block, "ep", self.up)

    def counter(self, block):
        return lax.ppermute(block, "ep", self.down)


def swap_section(block):
    return lax.ppermute(block, "section", [(0, 1), (1, 0)])


def prep_kernel(lengths, resid, gain, logits, routes, out, table):
    rows, width = out.shape[0], resid.shape[1]
    tok_rows = resid.shape[0]
    start = pl.multiple_of(lax.axis_index("section") * rows, rows)
    weights = logits[...]
    weights = weights / jnp.sum(weights, axis=0, keepdims=True)
    weights = weights.astype(jnp.bfloat16).astype(jnp.float32)
    chosen = routes[...]
    expert = lax.broadcasted_iota(jnp.int32, (LANES, tok_rows), 0)
    position = lax.broadcasted_iota(jnp.int32, (LANES, tok_rows), 1)
    mixed = jnp.zeros((LANES, tok_rows), jnp.float32)
    for k in range(chosen.shape[0]):
        mixed = mixed + jnp.where(expert == chosen[k : k + 1, :], weights[k : k + 1, :], 0.0)
    table[...] = jnp.where(position < lengths[0], mixed, 0.0).T
    out[:, width:] = table[pl.ds(start, rows), :].astype(jnp.bfloat16)
    values = resid[pl.ds(start, rows), :].astype(jnp.float32)
    mean_square = jnp.sum(values * values, axis=-1, keepdims=True) * (1.0 / width)
    gains = gain[...].astype(jnp.float32)
    gains = jnp.concatenate([gains[i : i + 1, :] for i in range(width // LANES)], axis=1)
    scaled = values * lax.rsqrt(mean_square + 1e-06) * gains
    out[:, :width] = scaled.astype(jnp.bfloat16)


def prep(lengths, resid, gain, logits, routes):
    tok_rows, width = resid.shape
    whole = pl.BlockSpec(memory_space=pltpu.VMEM)
    return pl.pallas_call(
        prep_kernel,
        out_shape=jax.ShapeDtypeStruct((tok_rows // 2, width + LANES), jnp.bfloat16),
        in_specs=[pl.BlockSpec(memory_space=pltpu.SMEM)] + [whole] * 4,
        out_specs=whole,
        scratch_shapes=[pltpu.VMEM((tok_rows, LANES), jnp.float32)],
        name="prep",
    )(lengths, resid, gain.reshape(width // LANES, LANES), logits.T, routes.T)


def gate_kernel(peer, *refs, count, tokens, width, local, levels):
    blocks = refs[:count]
    w_gate, w_up = refs[count : count + 2]
    active, spread, hold, gates, ups, picked, slot_t, block_sems, weight_sems = refs[-9:]
    copies = []
    start = 0
    for i, block in enumerate(blocks):
        rows = block.shape[0]
        copy = pltpu.make_async_copy(block, hold.at[pl.ds(start, rows), :], block_sems.at[i])
        copy.start()
        copies.append(copy)
        start += rows

    def weights(e):
        return (
            pltpu.make_async_copy(w_gate.at[e], gates.at[e], weight_sems.at[0, e]),
            pltpu.make_async_copy(w_up.at[e], ups.at[e], weight_sems.at[1, e]),
        )

    for copy in weights(0):
        copy.start()
    for copy in copies:
        copy.wait()
    if local > 1:
        for copy in weights(1):
            copy.start()

    lane_in = lax.broadcasted_iota(jnp.int32, (LANES, LANES), 0)
    lane_out = lax.broadcasted_iota(jnp.int32, (LANES, LANES), 1)
    pick = ((lane_in == peer[0] * local + lane_out) & (lane_out < local)).astype(jnp.bfloat16)
    earlier = (lane_out < lane_in).astype(jnp.bfloat16)
    carry = jnp.zeros((1, LANES), jnp.float32)
    capacity = levels * TILE
    column = lax.broadcasted_iota(jnp.int32, (LANES, capacity), 1).astype(jnp.float32)
    for b in range(tokens // LANES):
        span = slice(b * LANES, (b + 1) * LANES)
        mix = jnp.dot(hold[span, width:], pick, preferred_element_type=jnp.float32)
        hit = (mix > 0.0).astype(jnp.float32)
        rank = jnp.dot(earlier, hit.astype(jnp.bfloat16), preferred_element_type=jnp.float32)
        slot = jnp.where(mix > 0.0, rank + carry, -1.0)
        carry = carry + jnp.sum(hit, axis=0, keepdims=True)
        slot_t[:, span] = slot.T[: slot_t.shape[0], :]
        pieces = [
            jnp.where(slot[:, e : e + 1] == column, mix[:, e : e + 1], 0.0) for e in range(local)
        ]
        spread[span, :] = jnp.concatenate(pieces, axis=1).astype(jnp.bfloat16)

    def tile(level, e):
        row = lax.broadcasted_iota(jnp.int32, (TILE, tokens), 0) + level * TILE
        select = (slot_t[pl.ds(e, 1), :] == row.astype(jnp.float32)).astype(jnp.bfloat16)
        step = min(width, 1024)
        for k in range(width // step):
            span = slice(k * step, (k + 1) * step)
            picked[:, span] = jnp.dot(
                select, hold[:, span], preferred_element_type=jnp.float32
            ).astype(jnp.bfloat16)
        gate = jnp.dot(picked[...], gates[e], preferred_element_type=jnp.float32)
        up = jnp.dot(picked[...], ups[e], preferred_element_type=jnp.float32)
        value = gate / (1.0 + jnp.exp(-gate)) * up
        active[e, pl.ds(pl.multiple_of(level * TILE, 32), TILE), :] = value.astype(jnp.bfloat16)

    def expert(e, _):
        for copy in weights(e):
            copy.wait()

        @pl.when(e + 2 < local)
        def _():
            for copy in weights(e + 2):
                copy.start()

        if levels == 1:
            tile(0, e)
        else:
            lax.fori_loop(0, levels, lambda level, _: (tile(level, e), 0)[1], 0)
        return 0

    lax.fori_loop(0, local, expert, 0)


def gate_up(peer, blocks, w_gate, w_up, levels, after=()):
    local, width, units = w_gate.shape
    tokens = sum(block.shape[0] for block in blocks)
    hbm = pl.BlockSpec(memory_space=pl.ANY)
    vmem = pl.BlockSpec(memory_space=pltpu.VMEM)
    smem = pl.BlockSpec(memory_space=pltpu.SMEM)
    return pl.pallas_call(
        functools.partial(
            gate_kernel,
            count=len(blocks),
            tokens=tokens,
            width=width,
            local=local,
            levels=levels,
        ),
        in_specs=[smem] + [hbm] * (len(blocks) + 2 + len(after)),
        out_specs=[vmem, vmem],
        scratch_shapes=[
            pltpu.VMEM((tokens, width + LANES), jnp.bfloat16),
            pltpu.VMEM((local, width, units), jnp.bfloat16),
            pltpu.VMEM((local, width, units), jnp.bfloat16),
            pltpu.VMEM((TILE, width), jnp.bfloat16),
            pltpu.VMEM((max(8, local), tokens), jnp.float32),
            pltpu.SemaphoreType.DMA((len(blocks),)),
            pltpu.SemaphoreType.DMA((2, local)),
        ],
        out_shape=[
            jax.ShapeDtypeStruct((local, levels * TILE, units), jnp.bfloat16),
            jax.ShapeDtypeStruct((tokens, local * levels * TILE), jnp.bfloat16),
        ],
        compiler_params=pltpu.CompilerParams(vmem_limit_bytes=GATE_LIMIT),
        cost_estimate=pl.CostEstimate(
            flops=8_000_000_000, bytes_accessed=4 * local * width * units, transcendentals=0
        ),
        name="gate_up",
    )(peer, *blocks, w_gate, w_up, *after)


def down_kernel(half, active, spread, w_down, *rest):
    out, held = rest[-2:]
    local, capacity, _ = active.shape
    for e in range(local):
        held[e * capacity : (e + 1) * capacity, :] = jnp.dot(
            active[e], w_down[e], preferred_element_type=jnp.float32
        ).astype(jnp.bfloat16)
    out[...] = jnp.dot(spread[...], held[...], preferred_element_type=jnp.float32).astype(out.dtype)


def down_mix(half, active, spread, w_down, columns, dtype, after=(), step=512):
    local, capacity, units = active.shape
    tokens = spread.shape[0]
    steps = columns // step
    keep = lambda *shape: pl.BlockSpec(shape, lambda n, *_: (0,) * len(shape))
    return pl.pallas_call(
        down_kernel,
        grid_spec=pltpu.PrefetchScalarGridSpec(
            num_scalar_prefetch=1,
            grid=(steps,),
            in_specs=[
                keep(local, capacity, units),
                keep(tokens, local * capacity),
                pl.BlockSpec((local, units, step), lambda n, h: (0, 0, h[0] * steps + n)),
            ]
            + [pl.BlockSpec(memory_space=pl.ANY)] * len(after),
            out_specs=pl.BlockSpec((tokens, step), lambda n, h: (0, n)),
            scratch_shapes=[pltpu.VMEM((local * capacity, step), jnp.bfloat16)],
        ),
        out_shape=jax.ShapeDtypeStruct((tokens, columns), dtype),
        compiler_params=pltpu.CompilerParams(
            dimension_semantics=("arbitrary",), vmem_limit_bytes=DOWN_LIMIT
        ),
        cost_estimate=pl.CostEstimate(
            flops=3_000_000_000, bytes_accessed=2 * local * units * columns, transcendentals=0
        ),
        name="down_mix",
    )(half, active, spread, w_down, *after)


def gather_ring(ring, block):
    rows = block.shape[0] // 2
    behind, ahead = [block], [block]
    found = [[block]]
    for _ in range(1, ring.half):
        behind.append(ring.clockwise(behind[-1]))
        ahead.append(ring.counter(ahead[-1]))
        found += [[behind[-1]], [ahead[-1]]]
    far_up = ring.clockwise(behind[-1][:rows])
    far_down = ring.counter(ahead[-1][rows:])
    found.append([far_up, far_down])
    return found


def hop_kernel(*refs, plan):
    outs = refs[-len(plan) :]
    at = 0
    for out, (sides, held) in zip(outs, plan):
        rows = out.shape[0] // len(sides)
        count = len(sides)
        for i, side in enumerate(sides):
            value = refs[at + i][...].astype(jnp.float32)
            value = value + refs[at + count + i][...].astype(jnp.float32)
            if side in held:
                start = held.index(side) * rows
                acc = refs[at + 2 * count]
                value = value + acc[start : start + rows, :].astype(jnp.float32)
            out[i * rows : (i + 1) * rows, :] = value.astype(out.dtype)
        at += 2 * count + (1 if held else 0)


def hop_add(ways, count, column, rows, width):
    operands, specs, plan, shapes = [], [], [], []
    whole = lambda array: pl.BlockSpec(array.shape, lambda _: (0, 0))

    def view(side, place):
        return pl.BlockSpec((rows, width), lambda _: (side * count + place, column))

    for kept, taken, place, sides, acc, held in ways:
        operands += [kept] * len(sides) + [taken] * len(sides)
        specs += [view(side, place) for side in sides] + [view(1 - side, place) for side in sides]
        if held:
            operands.append(acc)
            specs.append(whole(acc))
        plan.append((sides, held))
        shapes.append(jax.ShapeDtypeStruct((len(sides) * rows, width), jnp.bfloat16))
    return pl.pallas_call(
        functools.partial(hop_kernel, plan=tuple(plan)),
        grid=(1,),
        in_specs=specs,
        out_specs=[whole(shape) for shape in shapes],
        out_shape=shapes,
        compiler_params=pltpu.CompilerParams(vmem_limit_bytes=SMALL_LIMIT),
        cost_estimate=pl.CostEstimate(
            flops=1_000_000_000, bytes_accessed=40 * rows * width, transcendentals=0
        ),
        name="hop_add",
    )(*operands)


def last_kernel(kept_0, kept_1, taken_0, taken_1, *refs):
    out = refs[-1]
    rows = kept_0.shape[0]
    width = refs[0].shape[1]
    section = lax.axis_index("section")
    for side, (kept, taken) in enumerate(((kept_0, taken_0), (kept_1, taken_1))):
        start = pl.multiple_of((side + section) % 2 * rows, rows)
        for column in range(len(refs) // 2):
            cols = slice(column * width, (column + 1) * width)
            value = kept[:, cols] + taken[:, cols].astype(jnp.float32)
            for acc in refs[2 * column : 2 * column + 2]:
                value = value + acc[side * rows : (side + 1) * rows, :].astype(jnp.float32)
            out[pl.ds(start, rows), cols] = value.astype(out.dtype)


def last_add(kept, taken, count, rows, arrived):
    total = kept.shape[1]
    view = lambda side: pl.BlockSpec((rows, total), lambda _: (side * count, 0))
    return pl.pallas_call(
        last_kernel,
        grid=(1,),
        in_specs=[view(0), view(1), view(1), view(0)]
        + [pl.BlockSpec(acc.shape, lambda _: (0, 0)) for acc in arrived],
        out_specs=pl.BlockSpec((2 * rows, total), lambda _: (0, 0)),
        out_shape=jax.ShapeDtypeStruct((2 * rows, total), jnp.bfloat16),
        compiler_params=pltpu.CompilerParams(vmem_limit_bytes=SMALL_LIMIT),
        name="last_add",
    )(kept, kept, taken, taken, *arrived)


def scatter_ring(ring, sums, rows, parts):
    count = ring.count // 2
    width = sums[0][0].shape[1] // parts

    moving = [[None, None] for _ in range(parts)]
    for hop in range(ring.half):
        for column in range(parts):
            ways = []
            for way in range(2):
                index = ring.count - 1 if hop == 0 else 2 * (ring.half - hop) - way
                sides = (way,) if hop == 0 else (0, 1)
                held = ((), (way,), (0, 1))[min(hop, 2)]
                kept, taken = sums[index // count]
                ways.append((kept, taken, index % count, sides, moving[column][way], held))
            blocks = hop_add(ways, count, column, rows, width)
            for way, move in enumerate((ring.clockwise, ring.counter)):
                moving[column][way] = move(blocks[way])
    arrived = [acc for pair in moving for acc in pair]
    return last_add(*sums[0], count, rows, arrived)


def kv_part(keys_raw, values_raw, k_gain, is_live, position, page_owner, page_slot):
    tok_rows, kv_width = keys_raw.shape
    head = k_gain.shape[0]
    pages = page_owner.shape[1]
    page = tok_rows // pages
    peer_count = lax.axis_size("ep")
    normed = rms_scale(
        keys_raw.astype(jnp.float32).reshape(tok_rows, kv_width // head, head),
        k_gain.astype(jnp.float32),
    )
    turned = rotate_keys(normed, position)
    key_rows = (
        jnp.where(is_live[:, None, None], turned, 0.0)
        .astype(jnp.bfloat16)
        .reshape(tok_rows, kv_width)
    )
    value_rows = jnp.where(is_live[:, None], values_raw, jnp.zeros_like(values_raw))
    page_rows = jnp.stack([key_rows, value_rows], axis=1).reshape(pages, page * 2 * kv_width)
    owners = page_owner.reshape(-1)
    same = (owners[:, None] == owners[None, :]) & (
        jnp.arange(pages)[None, :] < jnp.arange(pages)[:, None]
    )
    page_rank = jnp.sum(same.astype(jnp.int32), axis=1)
    lane_index = owners * PAGE_PEER + page_rank
    lane_ids = jnp.arange(peer_count * PAGE_PEER, dtype=jnp.int32)
    select = lane_ids[:, None] == lane_index[None, :]
    tagged = jnp.concatenate(
        [
            page_rows,
            jnp.broadcast_to(
                (page_slot.reshape(-1, 1) + 1).astype(jnp.bfloat16), (pages, LANES)
            ),
        ],
        axis=1,
    )
    sent = jnp.dot(
        select.astype(jnp.bfloat16), tagged, preferred_element_type=jnp.float32
    ).astype(jnp.bfloat16)
    sent = sent.reshape(peer_count, PAGE_PEER, tagged.shape[1])
    got = lax.all_to_all(sent, "ep", split_axis=0, concat_axis=0, tiled=True)
    got = got.reshape(peer_count * PAGE_PEER, tagged.shape[1])
    slots = got[:, -1].astype(jnp.int32) - 1
    placing = (jnp.arange(pages, dtype=jnp.int32)[:, None] == slots[None, :]).astype(jnp.bfloat16)
    cache = jnp.dot(placing, got[:, :-LANES], preferred_element_type=jnp.float32)
    return cache.astype(jnp.bfloat16).reshape(pages, page, 2, kv_width)


def shards(
    resid,
    norm_gain,
    gate_logits,
    routes,
    w_gate,
    w_up,
    w_down,
    keys_raw,
    values_raw,
    k_gain,
    lengths,
    page_owner,
    page_slot,
):
    tok_rows, model_width = resid.shape
    section_count = lax.axis_size("section")
    peer_count = lax.axis_size("ep")
    section = lax.axis_index("section")
    peer = lax.axis_index("ep").reshape(1).astype(jnp.int32)
    col_width = model_width // section_count
    ring = Ring(peer_count)
    position = jnp.arange(tok_rows, dtype=jnp.int32)
    is_live = position < lengths[0]

    kv_cache = kv_part(keys_raw, values_raw, k_gain, is_live, position, page_owner, page_slot)

    mine = section.reshape(1).astype(jnp.int32)
    near_count = peer_count // 2
    levels = -(-near_count * CAP // TILE)
    rows = tok_rows // section_count
    payload = prep(lengths, resid, norm_gain, gate_logits, routes)
    found = gather_ring(ring, payload)
    swapped = [[swap_section(piece) for piece in pieces] for pieces in found]
    groups = []
    for span in (slice(0, near_count), slice(near_count, peer_count)):
        blocks = [piece for pieces in found[span] + swapped[span] for piece in pieces]
        after = groups[-1][:1] if groups else ()
        groups.append(gate_up(peer, blocks, w_gate, w_up, levels, after))
    sums = [None, None]
    after = ()
    for group in (0, 1):
        active, spread = groups[group]
        given = down_mix(1 - mine, active, spread, w_down, col_width, jnp.bfloat16, after)
        taken = swap_section(given)
        kept = down_mix(mine, active, spread, w_down, col_width, jnp.float32, (given,))
        sums[group] = (kept, taken)
        after = (kept,)

    return (scatter_ring(ring, sums, rows, PARTS), kv_cache)


def solution(mesh):
    in_specs = (
        P(("groups", "ep"), None),
        P(),
        P(("groups", "ep"), None),
        P(("groups", "ep"), None),
        P("ep", None, "section"),
        P("ep", None, "section"),
        P("ep", "section", None),
        P(("groups", "ep"), "section"),
        P(("groups", "ep"), "section"),
        P(),
        P(("groups", "ep")),
        P(("groups", "ep"), None),
        P(("groups", "ep"), None),
    )
    out_specs = (P(("groups", "ep"), "section"), P(("groups", "ep"), None, None, "section"))

    return jax.shard_map(shards, mesh=mesh, in_specs=in_specs, out_specs=out_specs, check_vma=False)
```

```python
import functools
import math

import jax
import jax.numpy as jnp
from jax import lax
from jax.experimental import pallas as pl
from jax.experimental.pallas import tpu as pltpu
from jax.sharding import PartitionSpec as P


CAP = 40
PAGE_PEER = 2
LANES = 128
TILE = 160
PARTS = 2
SLOTS = 3
GATE_LIMIT = 48 * 1024 * 1024
DOWN_LIMIT = 44 * 1024 * 1024
SMALL_LIMIT = 12 * 1024 * 1024


def rms_scale(values, gain_row):
    mean_square = jnp.mean(values * values, axis=-1, keepdims=True)
    return values * lax.rsqrt(mean_square + 1e-06) * gain_row


def rotate_keys(key_block, position):
    half_size = key_block.shape[-1] // 2
    frequency = jnp.exp(
        jnp.arange(half_size, dtype=jnp.float32)
        * (-2.0 / key_block.shape[-1])
        * math.log(1000000.0)
    )
    angles = position.astype(jnp.float32)[:, None, None] * frequency
    cosine = jnp.cos(angles)
    sine_part = jnp.sin(angles)
    first_half = key_block[..., :half_size]
    second = key_block[..., half_size:]
    return jnp.concatenate(
        [first_half * cosine - second * sine_part, second * cosine + first_half * sine_part],
        axis=-1,
    )


class Ring:
    def __init__(self, count):
        order = list(range(0, count, 2)) + list(range(1, count, 2))[::-1]
        self.count = count
        self.half = count // 2
        self.up = [(order[i], order[(i + 1) % count]) for i in range(count)]
        self.down = [(b, a) for a, b in self.up]

    def clockwise(self, block):
        return lax.ppermute(block, "ep", self.up)

    def counter(self, block):
        return lax.ppermute(block, "ep", self.down)


def swap_section(block):
    return lax.ppermute(block, "section", [(0, 1), (1, 0)])


def prep_kernel(lengths, resid, gain, logits, routes, out, table):
    rows, width = out.shape[0], resid.shape[1]
    tok_rows = resid.shape[0]
    start = pl.multiple_of(lax.axis_index("section") * rows, rows)
    weights = logits[...]
    weights = weights / jnp.sum(weights, axis=0, keepdims=True)
    weights = weights.astype(jnp.bfloat16).astype(jnp.float32)
    chosen = routes[...]
    expert = lax.broadcasted_iota(jnp.int32, (LANES, tok_rows), 0)
    position = lax.broadcasted_iota(jnp.int32, (LANES, tok_rows), 1)
    mixed = jnp.zeros((LANES, tok_rows), jnp.float32)
    for k in range(chosen.shape[0]):
        mixed = mixed + jnp.where(expert == chosen[k : k + 1, :], weights[k : k + 1, :], 0.0)
    table[...] = jnp.where(position < lengths[0], mixed, 0.0).T
    out[:, width:] = table[pl.ds(start, rows), :].astype(jnp.bfloat16)
    values = resid[pl.ds(start, rows), :].astype(jnp.float32)
    mean_square = jnp.sum(values * values, axis=-1, keepdims=True) * (1.0 / width)
    gains = gain[...].astype(jnp.float32)
    gains = jnp.concatenate([gains[i : i + 1, :] for i in range(width // LANES)], axis=1)
    scaled = values * lax.rsqrt(mean_square + 1e-06) * gains
    out[:, :width] = scaled.astype(jnp.bfloat16)


def prep(lengths, resid, gain, logits, routes):
    tok_rows, width = resid.shape
    whole = pl.BlockSpec(memory_space=pltpu.VMEM)
    return pl.pallas_call(
        prep_kernel,
        out_shape=jax.ShapeDtypeStruct((tok_rows // 2, width + LANES), jnp.bfloat16),
        in_specs=[pl.BlockSpec(memory_space=pltpu.SMEM)] + [whole] * 4,
        out_specs=whole,
        scratch_shapes=[pltpu.VMEM((tok_rows, LANES), jnp.float32)],
        name="prep",
    )(lengths, resid, gain.reshape(width // LANES, LANES), logits.T, routes.T)


def gate_kernel(peer, *refs, count, tokens, width, local, levels):
    blocks = refs[:count]
    w_gate, w_up = refs[count : count + 2]
    active, spread, hold, gates, ups, picked, slot_t, block_sems, weight_sems = refs[-9:]
    slots = gates.shape[0]
    copies = []
    start = 0
    for i, block in enumerate(blocks):
        rows = block.shape[0]
        copy = pltpu.make_async_copy(block, hold.at[pl.ds(start, rows), :], block_sems.at[i])
        copy.start()
        copies.append(copy)
        start += rows

    def weights(e):
        return (
            pltpu.make_async_copy(w_gate.at[e], gates.at[e % slots], weight_sems.at[0, e]),
            pltpu.make_async_copy(w_up.at[e], ups.at[e % slots], weight_sems.at[1, e]),
        )

    for copy in weights(0):
        copy.start()
    for copy in copies:
        copy.wait()
    if local > 1:
        for copy in weights(1):
            copy.start()

    lane_in = lax.broadcasted_iota(jnp.int32, (LANES, LANES), 0)
    lane_out = lax.broadcasted_iota(jnp.int32, (LANES, LANES), 1)
    pick = ((lane_in == peer[0] * local + lane_out) & (lane_out < local)).astype(jnp.bfloat16)
    earlier = (lane_out < lane_in).astype(jnp.bfloat16)
    carry = jnp.zeros((1, LANES), jnp.float32)
    capacity = levels * TILE
    column = lax.broadcasted_iota(jnp.int32, (LANES, capacity), 1).astype(jnp.float32)
    for b in range(tokens // LANES):
        span = slice(b * LANES, (b + 1) * LANES)
        mix = jnp.dot(hold[span, width:], pick, preferred_element_type=jnp.float32)
        hit = (mix > 0.0).astype(jnp.float32)
        rank = jnp.dot(earlier, hit.astype(jnp.bfloat16), preferred_element_type=jnp.float32)
        slot = jnp.where(mix > 0.0, rank + carry, -1.0)
        carry = carry + jnp.sum(hit, axis=0, keepdims=True)
        slot_t[:, span] = slot.T[: slot_t.shape[0], :]
        pieces = [
            jnp.where(slot[:, e : e + 1] == column, mix[:, e : e + 1], 0.0) for e in range(local)
        ]
        spread[span, :] = jnp.concatenate(pieces, axis=1).astype(jnp.bfloat16)

    def tile(level, e):
        row = lax.broadcasted_iota(jnp.int32, (TILE, tokens), 0) + level * TILE
        select = (slot_t[pl.ds(e, 1), :] == row.astype(jnp.float32)).astype(jnp.bfloat16)
        step = min(width, 1024)
        for k in range(width // step):
            span = slice(k * step, (k + 1) * step)
            picked[:, span] = jnp.dot(
                select, hold[:, span], preferred_element_type=jnp.float32
            ).astype(jnp.bfloat16)
        gate = jnp.dot(picked[...], gates[e % slots], preferred_element_type=jnp.float32)
        up = jnp.dot(picked[...], ups[e % slots], preferred_element_type=jnp.float32)
        value = gate / (1.0 + jnp.exp(-gate)) * up
        active[e, pl.ds(pl.multiple_of(level * TILE, 32), TILE), :] = value.astype(jnp.bfloat16)

    def expert(e, _):
        for copy in weights(e):
            copy.wait()

        @pl.when(e + 2 < local)
        def _():
            for copy in weights(e + 2):
                copy.start()

        if levels == 1:
            tile(0, e)
        else:
            lax.fori_loop(0, levels, lambda level, _: (tile(level, e), 0)[1], 0)
        return 0

    lax.fori_loop(0, local, expert, 0)


def gate_up(peer, blocks, w_gate, w_up, levels, after=()):
    local, width, units = w_gate.shape
    tokens = sum(block.shape[0] for block in blocks)
    hbm = pl.BlockSpec(memory_space=pl.ANY)
    vmem = pl.BlockSpec(memory_space=pltpu.VMEM)
    smem = pl.BlockSpec(memory_space=pltpu.SMEM)
    return pl.pallas_call(
        functools.partial(
            gate_kernel,
            count=len(blocks),
            tokens=tokens,
            width=width,
            local=local,
            levels=levels,
        ),
        in_specs=[smem] + [hbm] * (len(blocks) + 2 + len(after)),
        out_specs=[vmem, vmem],
        scratch_shapes=[
            pltpu.VMEM((tokens, width + LANES), jnp.bfloat16),
            pltpu.VMEM((min(local, SLOTS), width, units), jnp.bfloat16),
            pltpu.VMEM((min(local, SLOTS), width, units), jnp.bfloat16),
            pltpu.VMEM((TILE, width), jnp.bfloat16),
            pltpu.VMEM((max(8, local), tokens), jnp.float32),
            pltpu.SemaphoreType.DMA((len(blocks),)),
            pltpu.SemaphoreType.DMA((2, local)),
        ],
        out_shape=[
            jax.ShapeDtypeStruct((local, levels * TILE, units), jnp.bfloat16),
            jax.ShapeDtypeStruct((tokens, local * levels * TILE), jnp.bfloat16),
        ],
        compiler_params=pltpu.CompilerParams(vmem_limit_bytes=GATE_LIMIT),
        cost_estimate=pl.CostEstimate(
            flops=8_000_000_000, bytes_accessed=4 * local * width * units, transcendentals=0
        ),
        name="gate_up",
    )(peer, *blocks, w_gate, w_up, *after)


def down_kernel(half, active, spread, w_down, *rest):
    out, held = rest[-2:]
    local, capacity, _ = active.shape
    for e in range(local):
        held[e * capacity : (e + 1) * capacity, :] = jnp.dot(
            active[e], w_down[e], preferred_element_type=jnp.float32
        ).astype(jnp.bfloat16)
    out[...] = jnp.dot(spread[...], held[...], preferred_element_type=jnp.float32).astype(out.dtype)


def down_mix(half, active, spread, w_down, columns, dtype, after=(), step=512):
    local, capacity, units = active.shape
    tokens = spread.shape[0]
    steps = columns // step
    keep = lambda *shape: pl.BlockSpec(shape, lambda n, *_: (0,) * len(shape))
    return pl.pallas_call(
        down_kernel,
        grid_spec=pltpu.PrefetchScalarGridSpec(
            num_scalar_prefetch=1,
            grid=(steps,),
            in_specs=[
                keep(local, capacity, units),
                keep(tokens, local * capacity),
                pl.BlockSpec((local, units, step), lambda n, h: (0, 0, h[0] * steps + n)),
            ]
            + [pl.BlockSpec(memory_space=pl.ANY)] * len(after),
            out_specs=pl.BlockSpec((tokens, step), lambda n, h: (0, n)),
            scratch_shapes=[pltpu.VMEM((local * capacity, step), jnp.bfloat16)],
        ),
        out_shape=jax.ShapeDtypeStruct((tokens, columns), dtype),
        compiler_params=pltpu.CompilerParams(
            dimension_semantics=("arbitrary",), vmem_limit_bytes=DOWN_LIMIT
        ),
        cost_estimate=pl.CostEstimate(
            flops=3_000_000_000, bytes_accessed=2 * local * units * columns, transcendentals=0
        ),
        name="down_mix",
    )(half, active, spread, w_down, *after)


def gather_ring(ring, block):
    rows = block.shape[0] // 2
    behind, ahead = [block], [block]
    found = [[block]]
    for _ in range(1, ring.half):
        behind.append(ring.clockwise(behind[-1]))
        ahead.append(ring.counter(ahead[-1]))
        found += [[behind[-1]], [ahead[-1]]]
    far_up = ring.clockwise(behind[-1][:rows])
    far_down = ring.counter(ahead[-1][rows:])
    found.append([far_up, far_down])
    return found


def hop_kernel(*refs, plan):
    outs = refs[-len(plan) :]
    at = 0
    for out, (sides, held) in zip(outs, plan):
        rows = out.shape[0] // len(sides)
        count = len(sides)
        for i, side in enumerate(sides):
            value = refs[at + i][...].astype(jnp.float32)
            value = value + refs[at + count + i][...].astype(jnp.float32)
            if side in held:
                start = held.index(side) * rows
                acc = refs[at + 2 * count]
                value = value + acc[start : start + rows, :].astype(jnp.float32)
            out[i * rows : (i + 1) * rows, :] = value.astype(out.dtype)
        at += 2 * count + (1 if held else 0)


def hop_add(ways, count, column, rows, width):
    operands, specs, plan, shapes = [], [], [], []
    whole = lambda array: pl.BlockSpec(array.shape, lambda _: (0, 0))

    def view(side, place):
        return pl.BlockSpec((rows, width), lambda _: (side * count + place, column))

    for kept, taken, place, sides, acc, held in ways:
        operands += [kept] * len(sides) + [taken] * len(sides)
        specs += [view(side, place) for side in sides] + [view(1 - side, place) for side in sides]
        if held:
            operands.append(acc)
            specs.append(whole(acc))
        plan.append((sides, held))
        shapes.append(jax.ShapeDtypeStruct((len(sides) * rows, width), jnp.bfloat16))
    return pl.pallas_call(
        functools.partial(hop_kernel, plan=tuple(plan)),
        grid=(1,),
        in_specs=specs,
        out_specs=[whole(shape) for shape in shapes],
        out_shape=shapes,
        compiler_params=pltpu.CompilerParams(vmem_limit_bytes=SMALL_LIMIT),
        cost_estimate=pl.CostEstimate(
            flops=1_000_000_000, bytes_accessed=40 * rows * width, transcendentals=0
        ),
        name="hop_add",
    )(*operands)


def last_kernel(kept_0, kept_1, taken_0, taken_1, *refs):
    out = refs[-1]
    rows = kept_0.shape[0]
    width = refs[0].shape[1]
    section = lax.axis_index("section")
    for side, (kept, taken) in enumerate(((kept_0, taken_0), (kept_1, taken_1))):
        start = pl.multiple_of((side + section) % 2 * rows, rows)
        for column in range(len(refs) // 2):
            cols = slice(column * width, (column + 1) * width)
            value = kept[:, cols].astype(jnp.float32) + taken[:, cols].astype(jnp.float32)
            for acc in refs[2 * column : 2 * column + 2]:
                value = value + acc[side * rows : (side + 1) * rows, :].astype(jnp.float32)
            out[pl.ds(start, rows), cols] = value.astype(out.dtype)


def last_add(kept, taken, count, rows, arrived):
    total = kept.shape[1]
    view = lambda side: pl.BlockSpec((rows, total), lambda _: (side * count, 0))
    return pl.pallas_call(
        last_kernel,
        grid=(1,),
        in_specs=[view(0), view(1), view(1), view(0)]
        + [pl.BlockSpec(acc.shape, lambda _: (0, 0)) for acc in arrived],
        out_specs=pl.BlockSpec((2 * rows, total), lambda _: (0, 0)),
        out_shape=jax.ShapeDtypeStruct((2 * rows, total), jnp.bfloat16),
        compiler_params=pltpu.CompilerParams(vmem_limit_bytes=SMALL_LIMIT),
        name="last_add",
    )(kept, kept, taken, taken, *arrived)


def scatter_ring(ring, sums, rows, parts):
    count = ring.count // 2
    width = sums[0][0].shape[1] // parts

    moving = [[None, None] for _ in range(parts)]
    for hop in range(ring.half):
        for column in range(parts):
            ways = []
            for way in range(2):
                index = ring.count - 1 if hop == 0 else 2 * (ring.half - hop) - way
                sides = (way,) if hop == 0 else (0, 1)
                held = ((), (way,), (0, 1))[min(hop, 2)]
                kept, taken = sums[index // count]
                ways.append((kept, taken, index % count, sides, moving[column][way], held))
            blocks = hop_add(ways, count, column, rows, width)
            for way, move in enumerate((ring.clockwise, ring.counter)):
                moving[column][way] = move(blocks[way])
    arrived = [acc for pair in moving for acc in pair]
    return last_add(*sums[0], count, rows, arrived)


def kv_part(keys_raw, values_raw, k_gain, is_live, position, page_owner, page_slot):
    tok_rows, kv_width = keys_raw.shape
    head = k_gain.shape[0]
    pages = page_owner.shape[1]
    page = tok_rows // pages
    peer_count = lax.axis_size("ep")
    normed = rms_scale(
        keys_raw.astype(jnp.float32).reshape(tok_rows, kv_width // head, head),
        k_gain.astype(jnp.float32),
    )
    turned = rotate_keys(normed, position)
    key_rows = (
        jnp.where(is_live[:, None, None], turned, 0.0)
        .astype(jnp.bfloat16)
        .reshape(tok_rows, kv_width)
    )
    value_rows = jnp.where(is_live[:, None], values_raw, jnp.zeros_like(values_raw))
    page_rows = jnp.stack([key_rows, value_rows], axis=1).reshape(pages, page * 2 * kv_width)
    owners = page_owner.reshape(-1)
    same = (owners[:, None] == owners[None, :]) & (
        jnp.arange(pages)[None, :] < jnp.arange(pages)[:, None]
    )
    page_rank = jnp.sum(same.astype(jnp.int32), axis=1)
    lane_index = owners * PAGE_PEER + page_rank
    lane_ids = jnp.arange(peer_count * PAGE_PEER, dtype=jnp.int32)
    select = lane_ids[:, None] == lane_index[None, :]
    tagged = jnp.concatenate(
        [
            page_rows,
            jnp.broadcast_to(
                (page_slot.reshape(-1, 1) + 1).astype(jnp.bfloat16), (pages, LANES)
            ),
        ],
        axis=1,
    )
    sent = jnp.dot(
        select.astype(jnp.bfloat16), tagged, preferred_element_type=jnp.float32
    ).astype(jnp.bfloat16)
    sent = sent.reshape(peer_count, PAGE_PEER, tagged.shape[1])
    got = lax.all_to_all(sent, "ep", split_axis=0, concat_axis=0, tiled=True)
    got = got.reshape(peer_count * PAGE_PEER, tagged.shape[1])
    slots = got[:, -1].astype(jnp.int32) - 1
    placing = (jnp.arange(pages, dtype=jnp.int32)[:, None] == slots[None, :]).astype(jnp.bfloat16)
    cache = jnp.dot(placing, got[:, :-LANES], preferred_element_type=jnp.float32)
    return cache.astype(jnp.bfloat16).reshape(pages, page, 2, kv_width)


def shards(
    resid,
    norm_gain,
    gate_logits,
    routes,
    w_gate,
    w_up,
    w_down,
    keys_raw,
    values_raw,
    k_gain,
    lengths,
    page_owner,
    page_slot,
):
    tok_rows, model_width = resid.shape
    section_count = lax.axis_size("section")
    peer_count = lax.axis_size("ep")
    section = lax.axis_index("section")
    peer = lax.axis_index("ep").reshape(1).astype(jnp.int32)
    col_width = model_width // section_count
    ring = Ring(peer_count)
    position = jnp.arange(tok_rows, dtype=jnp.int32)
    is_live = position < lengths[0]

    kv_cache = kv_part(keys_raw, values_raw, k_gain, is_live, position, page_owner, page_slot)

    mine = section.reshape(1).astype(jnp.int32)
    near_count = peer_count // 2
    levels = -(-near_count * CAP // TILE)
    rows = tok_rows // section_count
    payload = prep(lengths, resid, norm_gain, gate_logits, routes)
    found = gather_ring(ring, payload)
    swapped = [[swap_section(piece) for piece in pieces] for pieces in found]
    groups = []
    for span in (slice(0, near_count), slice(near_count, peer_count)):
        blocks = [piece for pieces in found[span] + swapped[span] for piece in pieces]
        after = groups[-1][:1] if groups else ()
        groups.append(gate_up(peer, blocks, w_gate, w_up, levels, after))
    sums = [None, None]
    after = ()
    for group in (0, 1):
        active, spread = groups[group]
        given = down_mix(1 - mine, active, spread, w_down, col_width, jnp.bfloat16, after)
        taken = swap_section(given)
        kept = down_mix(mine, active, spread, w_down, col_width, jnp.bfloat16, (given,))
        sums[group] = (kept, taken)
        after = (kept,)

    return (scatter_ring(ring, sums, rows, PARTS), kv_cache)


def solution(mesh):
    in_specs = (
        P(("groups", "ep"), None),
        P(),
        P(("groups", "ep"), None),
        P(("groups", "ep"), None),
        P("ep", None, "section"),
        P("ep", None, "section"),
        P("ep", "section", None),
        P(("groups", "ep"), "section"),
        P(("groups", "ep"), "section"),
        P(),
        P(("groups", "ep")),
        P(("groups", "ep"), None),
        P(("groups", "ep"), None),
    )
    out_specs = (P(("groups", "ep"), "section"), P(("groups", "ep"), None, None, "section"))

    return jax.shard_map(shards, mesh=mesh, in_specs=in_specs, out_specs=out_specs, check_vma=False)
```

```python
import functools
import math

import jax
import jax.numpy as jnp
from jax import lax
from jax.experimental import pallas as pl
from jax.experimental.pallas import tpu as pltpu
from jax.sharding import PartitionSpec as P


CAP = 40
PAGE_PEER = 2
LANES = 128
TILE = 160
PARTS = 2
SLOTS = 3
GATE_LIMIT = 48 * 1024 * 1024
DOWN_LIMIT = 44 * 1024 * 1024
SMALL_LIMIT = 12 * 1024 * 1024


def rms_scale(values, gain_row):
    mean_square = jnp.mean(values * values, axis=-1, keepdims=True)
    return values * lax.rsqrt(mean_square + 1e-06) * gain_row


def rotate_keys(key_block, position):
    half_size = key_block.shape[-1] // 2
    frequency = jnp.exp(
        jnp.arange(half_size, dtype=jnp.float32)
        * (-2.0 / key_block.shape[-1])
        * math.log(1000000.0)
    )
    angles = position.astype(jnp.float32)[:, None, None] * frequency
    cosine = jnp.cos(angles)
    sine_part = jnp.sin(angles)
    first_half = key_block[..., :half_size]
    second = key_block[..., half_size:]
    return jnp.concatenate(
        [first_half * cosine - second * sine_part, second * cosine + first_half * sine_part],
        axis=-1,
    )


class Ring:
    def __init__(self, count):
        order = list(range(0, count, 2)) + list(range(1, count, 2))[::-1]
        self.count = count
        self.half = count // 2
        self.up = [(order[i], order[(i + 1) % count]) for i in range(count)]
        self.down = [(b, a) for a, b in self.up]

    def clockwise(self, block):
        return lax.ppermute(block, "ep", self.up)

    def counter(self, block):
        return lax.ppermute(block, "ep", self.down)


def swap_section(block):
    return lax.ppermute(block, "section", [(0, 1), (1, 0)])


def prep_kernel(lengths, resid, gain, logits, routes, out, table):
    rows, width = out.shape[0], resid.shape[1]
    tok_rows = resid.shape[0]
    start = pl.multiple_of(lax.axis_index("section") * rows, rows)
    weights = logits[...]
    weights = weights / jnp.sum(weights, axis=0, keepdims=True)
    weights = weights.astype(jnp.bfloat16).astype(jnp.float32)
    chosen = routes[...]
    expert = lax.broadcasted_iota(jnp.int32, (LANES, tok_rows), 0)
    position = lax.broadcasted_iota(jnp.int32, (LANES, tok_rows), 1)
    mixed = jnp.zeros((LANES, tok_rows), jnp.float32)
    for k in range(chosen.shape[0]):
        mixed = mixed + jnp.where(expert == chosen[k : k + 1, :], weights[k : k + 1, :], 0.0)
    table[...] = jnp.where(position < lengths[0], mixed, 0.0).T
    out[:, width:] = table[pl.ds(start, rows), :].astype(jnp.bfloat16)
    values = resid[pl.ds(start, rows), :].astype(jnp.float32)
    mean_square = jnp.sum(values * values, axis=-1, keepdims=True) * (1.0 / width)
    gains = gain[...].astype(jnp.float32)
    gains = jnp.concatenate([gains[i : i + 1, :] for i in range(width // LANES)], axis=1)
    scaled = values * lax.rsqrt(mean_square + 1e-06) * gains
    out[:, :width] = scaled.astype(jnp.bfloat16)


def prep(lengths, resid, gain, logits, routes):
    tok_rows, width = resid.shape
    whole = pl.BlockSpec(memory_space=pltpu.VMEM)
    return pl.pallas_call(
        prep_kernel,
        out_shape=jax.ShapeDtypeStruct((tok_rows // 2, width + LANES), jnp.bfloat16),
        in_specs=[pl.BlockSpec(memory_space=pltpu.SMEM)] + [whole] * 4,
        out_specs=whole,
        scratch_shapes=[pltpu.VMEM((tok_rows, LANES), jnp.float32)],
        name="prep",
    )(lengths, resid, gain.reshape(width // LANES, LANES), logits.T, routes.T)


def gate_kernel(peer, *refs, count, tokens, width, local, levels):
    blocks = refs[:count]
    w_gate, w_up = refs[count : count + 2]
    active, spread, hold, gates, ups, picked, slot_t, block_sems, weight_sems = refs[-9:]
    slots = gates.shape[0]
    copies = []
    start = 0
    for i, block in enumerate(blocks):
        rows = block.shape[0]
        copy = pltpu.make_async_copy(block, hold.at[pl.ds(start, rows), :], block_sems.at[i])
        copy.start()
        copies.append(copy)
        start += rows

    def weights(e):
        return (
            pltpu.make_async_copy(w_gate.at[e], gates.at[e % slots], weight_sems.at[0, e]),
            pltpu.make_async_copy(w_up.at[e], ups.at[e % slots], weight_sems.at[1, e]),
        )

    for copy in weights(0):
        copy.start()
    for copy in copies:
        copy.wait()
    if local > 1:
        for copy in weights(1):
            copy.start()

    lane_in = lax.broadcasted_iota(jnp.int32, (LANES, LANES), 0)
    lane_out = lax.broadcasted_iota(jnp.int32, (LANES, LANES), 1)
    pick = ((lane_in == peer[0] * local + lane_out) & (lane_out < local)).astype(jnp.bfloat16)
    earlier = (lane_out < lane_in).astype(jnp.bfloat16)
    carry = jnp.zeros((1, LANES), jnp.float32)
    capacity = levels * TILE
    column = lax.broadcasted_iota(jnp.int32, (LANES, capacity), 1).astype(jnp.float32)
    for b in range(tokens // LANES):
        span = slice(b * LANES, (b + 1) * LANES)
        mix = jnp.dot(hold[span, width:], pick, preferred_element_type=jnp.float32)
        hit = (mix > 0.0).astype(jnp.float32)
        rank = jnp.dot(earlier, hit.astype(jnp.bfloat16), preferred_element_type=jnp.float32)
        slot = jnp.where(mix > 0.0, rank + carry, -1.0)
        carry = carry + jnp.sum(hit, axis=0, keepdims=True)
        slot_t[:, span] = slot.T[: slot_t.shape[0], :]
        pieces = [
            jnp.where(slot[:, e : e + 1] == column, mix[:, e : e + 1], 0.0) for e in range(local)
        ]
        spread[span, :] = jnp.concatenate(pieces, axis=1).astype(jnp.bfloat16)

    def tile(level, e):
        row = lax.broadcasted_iota(jnp.int32, (TILE, tokens), 0) + level * TILE
        select = (slot_t[pl.ds(e, 1), :] == row.astype(jnp.float32)).astype(jnp.bfloat16)
        step = min(width, 1024)
        for k in range(width // step):
            span = slice(k * step, (k + 1) * step)
            picked[:, span] = jnp.dot(
                select, hold[:, span], preferred_element_type=jnp.float32
            ).astype(jnp.bfloat16)
        gate = jnp.dot(picked[...], gates[e % slots], preferred_element_type=jnp.float32)
        up = jnp.dot(picked[...], ups[e % slots], preferred_element_type=jnp.float32)
        value = gate / (1.0 + jnp.exp(-gate)) * up
        active[e, pl.ds(pl.multiple_of(level * TILE, 32), TILE), :] = value.astype(jnp.bfloat16)

    def expert(e, _):
        for copy in weights(e):
            copy.wait()

        @pl.when(e + 2 < local)
        def _():
            for copy in weights(e + 2):
                copy.start()

        if levels == 1:
            tile(0, e)
        else:
            lax.fori_loop(0, levels, lambda level, _: (tile(level, e), 0)[1], 0)
        return 0

    lax.fori_loop(0, local, expert, 0)


def gate_up(peer, blocks, w_gate, w_up, levels, after=()):
    local, width, units = w_gate.shape
    tokens = sum(block.shape[0] for block in blocks)
    hbm = pl.BlockSpec(memory_space=pl.ANY)
    vmem = pl.BlockSpec(memory_space=pltpu.VMEM)
    smem = pl.BlockSpec(memory_space=pltpu.SMEM)
    return pl.pallas_call(
        functools.partial(
            gate_kernel,
            count=len(blocks),
            tokens=tokens,
            width=width,
            local=local,
            levels=levels,
        ),
        in_specs=[smem] + [hbm] * (len(blocks) + 2 + len(after)),
        out_specs=[vmem, vmem],
        scratch_shapes=[
            pltpu.VMEM((tokens, width + LANES), jnp.bfloat16),
            pltpu.VMEM((min(local, SLOTS), width, units), jnp.bfloat16),
            pltpu.VMEM((min(local, SLOTS), width, units), jnp.bfloat16),
            pltpu.VMEM((TILE, width), jnp.bfloat16),
            pltpu.VMEM((max(8, local), tokens), jnp.float32),
            pltpu.SemaphoreType.DMA((len(blocks),)),
            pltpu.SemaphoreType.DMA((2, local)),
        ],
        out_shape=[
            jax.ShapeDtypeStruct((local, levels * TILE, units), jnp.bfloat16),
            jax.ShapeDtypeStruct((tokens, local * levels * TILE), jnp.bfloat16),
        ],
        compiler_params=pltpu.CompilerParams(vmem_limit_bytes=GATE_LIMIT),
        cost_estimate=pl.CostEstimate(
            flops=8_000_000_000, bytes_accessed=4 * local * width * units, transcendentals=0
        ),
        name="gate_up",
    )(peer, *blocks, w_gate, w_up, *after)


def down_kernel(half, active, spread, w_down, *rest):
    out, held = rest[-2:]
    local, capacity, _ = active.shape
    for e in range(local):
        held[e * capacity : (e + 1) * capacity, :] = jnp.dot(
            active[e], w_down[e], preferred_element_type=jnp.float32
        ).astype(jnp.bfloat16)
    out[...] = jnp.dot(spread[...], held[...], preferred_element_type=jnp.float32).astype(out.dtype)


def down_mix(half, active, spread, w_down, columns, dtype, after=(), step=1024):
    local, capacity, units = active.shape
    tokens = spread.shape[0]
    steps = columns // step
    keep = lambda *shape: pl.BlockSpec(shape, lambda n, *_: (0,) * len(shape))
    return pl.pallas_call(
        down_kernel,
        grid_spec=pltpu.PrefetchScalarGridSpec(
            num_scalar_prefetch=1,
            grid=(steps,),
            in_specs=[
                keep(local, capacity, units),
                keep(tokens, local * capacity),
                pl.BlockSpec((local, units, step), lambda n, h: (0, 0, h[0] * steps + n)),
            ]
            + [pl.BlockSpec(memory_space=pl.ANY)] * len(after),
            out_specs=pl.BlockSpec((tokens, step), lambda n, h: (0, n)),
            scratch_shapes=[pltpu.VMEM((local * capacity, step), jnp.bfloat16)],
        ),
        out_shape=jax.ShapeDtypeStruct((tokens, columns), dtype),
        compiler_params=pltpu.CompilerParams(
            dimension_semantics=("arbitrary",), vmem_limit_bytes=DOWN_LIMIT
        ),
        cost_estimate=pl.CostEstimate(
            flops=3_000_000_000, bytes_accessed=2 * local * units * columns, transcendentals=0
        ),
        name="down_mix",
    )(half, active, spread, w_down, *after)


def gather_ring(ring, block):
    rows = block.shape[0] // 2
    behind, ahead = [block], [block]
    found = [[block]]
    for _ in range(1, ring.half):
        behind.append(ring.clockwise(behind[-1]))
        ahead.append(ring.counter(ahead[-1]))
        found += [[behind[-1]], [ahead[-1]]]
    far_up = ring.clockwise(behind[-1][:rows])
    far_down = ring.counter(ahead[-1][rows:])
    found.append([far_up, far_down])
    return found


def hop_kernel(*refs, plan):
    outs = refs[-len(plan) :]
    at = 0
    for out, (sides, held) in zip(outs, plan):
        rows = out.shape[0] // len(sides)
        count = len(sides)
        for i, side in enumerate(sides):
            value = refs[at + i][...].astype(jnp.float32)
            value = value + refs[at + count + i][...].astype(jnp.float32)
            if side in held:
                start = held.index(side) * rows
                acc = refs[at + 2 * count]
                value = value + acc[start : start + rows, :].astype(jnp.float32)
            out[i * rows : (i + 1) * rows, :] = value.astype(out.dtype)
        at += 2 * count + (1 if held else 0)


def hop_add(ways, count, column, rows, width):
    operands, specs, plan, shapes = [], [], [], []
    whole = lambda array: pl.BlockSpec(array.shape, lambda _: (0, 0))

    def view(side, place):
        return pl.BlockSpec((rows, width), lambda _: (side * count + place, column))

    for kept, taken, place, sides, acc, held in ways:
        operands += [kept] * len(sides) + [taken] * len(sides)
        specs += [view(side, place) for side in sides] + [view(1 - side, place) for side in sides]
        if held:
            operands.append(acc)
            specs.append(whole(acc))
        plan.append((sides, held))
        shapes.append(jax.ShapeDtypeStruct((len(sides) * rows, width), jnp.bfloat16))
    return pl.pallas_call(
        functools.partial(hop_kernel, plan=tuple(plan)),
        grid=(1,),
        in_specs=specs,
        out_specs=[whole(shape) for shape in shapes],
        out_shape=shapes,
        compiler_params=pltpu.CompilerParams(vmem_limit_bytes=SMALL_LIMIT),
        cost_estimate=pl.CostEstimate(
            flops=1_000_000_000, bytes_accessed=40 * rows * width, transcendentals=0
        ),
        name="hop_add",
    )(*operands)


def last_kernel(kept_0, kept_1, taken_0, taken_1, *refs):
    out = refs[-1]
    rows = kept_0.shape[0]
    width = refs[0].shape[1]
    section = lax.axis_index("section")
    for side, (kept, taken) in enumerate(((kept_0, taken_0), (kept_1, taken_1))):
        start = pl.multiple_of((side + section) % 2 * rows, rows)
        for column in range(len(refs) // 2):
            cols = slice(column * width, (column + 1) * width)
            value = kept[:, cols].astype(jnp.float32) + taken[:, cols].astype(jnp.float32)
            for acc in refs[2 * column : 2 * column + 2]:
                value = value + acc[side * rows : (side + 1) * rows, :].astype(jnp.float32)
            out[pl.ds(start, rows), cols] = value.astype(out.dtype)


def last_add(kept, taken, count, rows, arrived):
    total = kept.shape[1]
    view = lambda side: pl.BlockSpec((rows, total), lambda _: (side * count, 0))
    return pl.pallas_call(
        last_kernel,
        grid=(1,),
        in_specs=[view(0), view(1), view(1), view(0)]
        + [pl.BlockSpec(acc.shape, lambda _: (0, 0)) for acc in arrived],
        out_specs=pl.BlockSpec((2 * rows, total), lambda _: (0, 0)),
        out_shape=jax.ShapeDtypeStruct((2 * rows, total), jnp.bfloat16),
        compiler_params=pltpu.CompilerParams(vmem_limit_bytes=SMALL_LIMIT),
        name="last_add",
    )(kept, kept, taken, taken, *arrived)


def scatter_ring(ring, sums, rows, parts):
    count = ring.count // 2
    width = sums[0][0].shape[1] // parts

    moving = [[None, None] for _ in range(parts)]
    for hop in range(ring.half):
        for column in range(parts):
            ways = []
            for way in range(2):
                index = ring.count - 1 if hop == 0 else 2 * (ring.half - hop) - way
                sides = (way,) if hop == 0 else (0, 1)
                held = ((), (way,), (0, 1))[min(hop, 2)]
                kept, taken = sums[index // count]
                ways.append((kept, taken, index % count, sides, moving[column][way], held))
            blocks = hop_add(ways, count, column, rows, width)
            for way, move in enumerate((ring.clockwise, ring.counter)):
                moving[column][way] = move(blocks[way])
    arrived = [acc for pair in moving for acc in pair]
    return last_add(*sums[0], count, rows, arrived)


def kv_part(keys_raw, values_raw, k_gain, is_live, position, page_owner, page_slot):
    tok_rows, kv_width = keys_raw.shape
    head = k_gain.shape[0]
    pages = page_owner.shape[1]
    page = tok_rows // pages
    peer_count = lax.axis_size("ep")
    normed = rms_scale(
        keys_raw.astype(jnp.float32).reshape(tok_rows, kv_width // head, head),
        k_gain.astype(jnp.float32),
    )
    turned = rotate_keys(normed, position)
    key_rows = (
        jnp.where(is_live[:, None, None], turned, 0.0)
        .astype(jnp.bfloat16)
        .reshape(tok_rows, kv_width)
    )
    value_rows = jnp.where(is_live[:, None], values_raw, jnp.zeros_like(values_raw))
    page_rows = jnp.stack([key_rows, value_rows], axis=1).reshape(pages, page * 2 * kv_width)
    owners = page_owner.reshape(-1)
    same = (owners[:, None] == owners[None, :]) & (
        jnp.arange(pages)[None, :] < jnp.arange(pages)[:, None]
    )
    page_rank = jnp.sum(same.astype(jnp.int32), axis=1)
    lane_index = owners * PAGE_PEER + page_rank
    lane_ids = jnp.arange(peer_count * PAGE_PEER, dtype=jnp.int32)
    select = lane_ids[:, None] == lane_index[None, :]
    tagged = jnp.concatenate(
        [
            page_rows,
            jnp.broadcast_to(
                (page_slot.reshape(-1, 1) + 1).astype(jnp.bfloat16), (pages, LANES)
            ),
        ],
        axis=1,
    )
    sent = jnp.dot(
        select.astype(jnp.bfloat16), tagged, preferred_element_type=jnp.float32
    ).astype(jnp.bfloat16)
    sent = sent.reshape(peer_count, PAGE_PEER, tagged.shape[1])
    got = lax.all_to_all(sent, "ep", split_axis=0, concat_axis=0, tiled=True)
    got = got.reshape(peer_count * PAGE_PEER, tagged.shape[1])
    slots = got[:, -1].astype(jnp.int32) - 1
    placing = (jnp.arange(pages, dtype=jnp.int32)[:, None] == slots[None, :]).astype(jnp.bfloat16)
    cache = jnp.dot(placing, got[:, :-LANES], preferred_element_type=jnp.float32)
    return cache.astype(jnp.bfloat16).reshape(pages, page, 2, kv_width)


def shards(
    resid,
    norm_gain,
    gate_logits,
    routes,
    w_gate,
    w_up,
    w_down,
    keys_raw,
    values_raw,
    k_gain,
    lengths,
    page_owner,
    page_slot,
):
    tok_rows, model_width = resid.shape
    section_count = lax.axis_size("section")
    peer_count = lax.axis_size("ep")
    section = lax.axis_index("section")
    peer = lax.axis_index("ep").reshape(1).astype(jnp.int32)
    col_width = model_width // section_count
    ring = Ring(peer_count)
    position = jnp.arange(tok_rows, dtype=jnp.int32)
    is_live = position < lengths[0]

    kv_cache = kv_part(keys_raw, values_raw, k_gain, is_live, position, page_owner, page_slot)

    mine = section.reshape(1).astype(jnp.int32)
    near_count = peer_count // 2
    levels = -(-near_count * CAP // TILE)
    rows = tok_rows // section_count
    payload = prep(lengths, resid, norm_gain, gate_logits, routes)
    found = gather_ring(ring, payload)
    swapped = [[swap_section(piece) for piece in pieces] for pieces in found]
    groups = []
    for span in (slice(0, near_count), slice(near_count, peer_count)):
        blocks = [piece for pieces in found[span] + swapped[span] for piece in pieces]
        after = groups[-1][:1] if groups else ()
        groups.append(gate_up(peer, blocks, w_gate, w_up, levels, after))

    def half_sums(side, group, after):
        active, spread = groups[group]
        return down_mix(side, active, spread, w_down, col_width, jnp.bfloat16, after)

    given_near = half_sums(1 - mine, 0, ())
    given_far = half_sums(1 - mine, 1, (given_near,))
    kept_far = half_sums(mine, 1, (given_far,))
    kept_near = half_sums(mine, 0, (kept_far,))
    taken_near = swap_section(given_near)
    taken_far = swap_section(given_far)
    sums = [(kept_near, taken_near), (kept_far, taken_far)]
    return (scatter_ring(ring, sums, rows, PARTS), kv_cache)


def solution(mesh):
    in_specs = (
        P(("groups", "ep"), None),
        P(),
        P(("groups", "ep"), None),
        P(("groups", "ep"), None),
        P("ep", None, "section"),
        P("ep", None, "section"),
        P("ep", "section", None),
        P(("groups", "ep"), "section"),
        P(("groups", "ep"), "section"),
        P(),
        P(("groups", "ep")),
        P(("groups", "ep"), None),
        P(("groups", "ep"), None),
    )
    out_specs = (P(("groups", "ep"), "section"), P(("groups", "ep"), None, None, "section"))

    return jax.shard_map(shards, mesh=mesh, in_specs=in_specs, out_specs=out_specs, check_vma=False)
```
